128 devices in a mesh: tp: 2 (over core), dp: 64 (over z, y, x).
Axes of the slice: x: 4, y: 4, z: 4, core: 2. Of those that a mesh axis runs over, the one named last changes fastest.
Arguments:
- hidden: bfloat16 [128, 64, 3072], P('dp')
- positions: int32 [64], replicated
- ln1_gain: bfloat16 [3072], replicated
- ln1_bias: bfloat16 [3072], replicated
- w_q: bfloat16 [3072, 3072], P(None, 'tp')
- w_k: bfloat16 [3072, 1024], P(None, 'tp')
- w_v: bfloat16 [3072, 1024], P(None, 'tp')
- w_o: bfloat16 [3072, 3072], P('tp')
- ln2_gain: bfloat16 [3072], replicated
- ln2_bias: bfloat16 [3072], replicated
- w_up: bfloat16 [3072, 9216], P(None, 'tp')
- w_down: bfloat16 [9216, 3072], P('tp')
Outputs:
- output 1: bfloat16 [128, 64, 3072], P('dp')
- output 2: float32 [9216], P('tp')
- output 3: float32 [24], P('tp')
- output 4: float32 [3072], replicated
All inputs are finite; a program needn't handle non-finite values.
Results may differ from the reference program's by a relative error of at most 0.00804819.
Values sent between devices are 32-bit elements.
A program may use at most 1 GiB of HBM per device.

```python
import jax
import jax.numpy as jnp
from jax import lax

D = 3072
HEADS = 24
KV_HEADS = 8
HEAD = 128
FF = 9216
SAMPLES = 128
SEQ_LEN = 64
POS_GAP = 64
ROT_DIM = HEAD // 2
ROPE_BASE = 10000.0
LN_EPS = 1e-5


def setup_inputs(seed: int = 0) -> dict:
    key_list = jax.random.split(jax.random.key(seed), 13)
    sample_shift = jax.random.normal(key_list[0], (SAMPLES, 1, D), jnp.float32)
    token_noise = jax.random.normal(key_list[1], (SAMPLES, SEQ_LEN, D), jnp.float32)
    hidden = (0.8 * sample_shift + 0.6 * token_noise).astype(jnp.bfloat16)
    pos_gaps = jax.random.randint(key_list[2], (SEQ_LEN,), 1, POS_GAP + 1)
    positions = (jnp.cumsum(pos_gaps) - pos_gaps[0]).astype(jnp.int32)

    def normal_weight(key_w, rows_in, cols_out):
        return (jax.random.normal(key_w, (rows_in, cols_out), jnp.float32) * rows_in ** -0.5).astype(jnp.bfloat16)

    def norm_param(key_w):
        return (0.3 * jax.random.normal(key_w, (D,), jnp.float32)).astype(jnp.bfloat16)

    return {
        "hidden": hidden,
        "positions": positions,
        "ln1_gain": norm_param(key_list[3]),
        "ln1_bias": norm_param(key_list[4]),
        "w_q": normal_weight(key_list[5], D, HEADS * HEAD),
        "w_k": normal_weight(key_list[6], D, KV_HEADS * HEAD),
        "w_v": normal_weight(key_list[7], D, KV_HEADS * HEAD),
        "w_o": normal_weight(key_list[8], HEADS * HEAD, D),
        "ln2_gain": norm_param(key_list[9]),
        "ln2_bias": norm_param(key_list[10]),
        "w_up": normal_weight(key_list[11], D, FF),
        "w_down": normal_weight(key_list[12], FF, D),
    }


def layer_norm_1p(in_rows, ln_gain, ln_bias):
    rows_f32 = in_rows.astype(jnp.float32)
    row_mean = jnp.mean(rows_f32, axis=-1, keepdims=True)
    centered = rows_f32 - row_mean
    row_var = jnp.mean(centered * centered, axis=-1, keepdims=True)
    scaled = centered * lax.rsqrt(row_var + LN_EPS)
    return (scaled * (1.0 + ln_gain.astype(jnp.float32)) + ln_bias.astype(jnp.float32)).astype(jnp.bfloat16)


def rope_tables(positions):
    rot_half = ROT_DIM // 2
    inv_freq = ROPE_BASE ** (-2.0 * jnp.arange(rot_half, dtype=jnp.float32) / ROT_DIM)
    pos_angle = positions.astype(jnp.float32)[:, None] * inv_freq[None, :]
    return jnp.cos(pos_angle), jnp.sin(pos_angle)


def apply_rope(heads_in, cos_b, sin_b):
    rot_half = ROT_DIM // 2
    heads_f32 = heads_in.astype(jnp.float32)
    lead_half = heads_f32[..., :rot_half]
    tail_half = heads_f32[..., rot_half:ROT_DIM]
    turned = jnp.concatenate([lead_half * cos_b - tail_half * sin_b, tail_half * cos_b + lead_half * sin_b], axis=-1)
    return jnp.concatenate([turned.astype(jnp.bfloat16), heads_in[..., ROT_DIM:]], axis=-1)


def reference(hidden, positions, ln1_gain, ln1_bias, w_q, w_k, w_v, w_o, ln2_gain, ln2_bias, w_up, w_down):
    q_group = HEADS // KV_HEADS
    cos_t, sin_t = rope_tables(positions)
    cos_b = cos_t[:, None, :]
    sin_b = sin_t[:, None, :]
    causal = jnp.arange(SEQ_LEN)[:, None] >= jnp.arange(SEQ_LEN)[None, :]

    def one_sample(x_rows):
        h_in = layer_norm_1p(x_rows, ln1_gain, ln1_bias)
        q_proj = jnp.dot(h_in, w_q, preferred_element_type=jnp.float32).astype(jnp.bfloat16).reshape(SEQ_LEN, HEADS, HEAD)
        k_proj = jnp.dot(h_in, w_k, preferred_element_type=jnp.float32).astype(jnp.bfloat16).reshape(SEQ_LEN, KV_HEADS, HEAD)
        v_proj = jnp.dot(h_in, w_v, preferred_element_type=jnp.float32).astype(jnp.bfloat16).reshape(SEQ_LEN, KV_HEADS, HEAD)
        q_proj = apply_rope(q_proj, cos_b, sin_b)
        k_proj = apply_rope(k_proj, cos_b, sin_b)
        k_full = jnp.repeat(k_proj, q_group, axis=1)
        v_full = jnp.repeat(v_proj, q_group, axis=1)
        scores = jnp.einsum("qhd,khd->hqk", q_proj.astype(jnp.float32), k_full.astype(jnp.float32)) * HEAD ** -0.5
        scores = jnp.where(causal[None, :, :], scores, -1e30)
        attn_prob = jax.nn.softmax(scores, axis=-1).astype(jnp.bfloat16)
        attn_out = jnp.einsum("hqk,khd->qhd", attn_prob.astype(jnp.float32), v_full.astype(jnp.float32)).astype(jnp.bfloat16)
        head_norm = jnp.sqrt(jnp.sum(jnp.square(attn_out.astype(jnp.float32)), axis=-1))
        o_sum = jnp.dot(attn_out.reshape(SEQ_LEN, HEADS * HEAD), w_o, preferred_element_type=jnp.float32)
        x_mid = (x_rows.astype(jnp.float32) + o_sum).astype(jnp.bfloat16)
        h_mid = layer_norm_1p(x_mid, ln2_gain, ln2_bias)
        mlp_act = jnp.square(jax.nn.relu(jnp.dot(h_mid, w_up, preferred_element_type=jnp.float32)))
        mlp_sum = jnp.dot(mlp_act.astype(jnp.bfloat16), w_down, preferred_element_type=jnp.float32)
        out_rows = (x_mid.astype(jnp.float32) + mlp_sum).astype(jnp.bfloat16)
        sample_means = (
            jnp.mean(mlp_act, axis=0),
            jnp.mean(head_norm, axis=0),
            jnp.mean(h_in.astype(jnp.float32), axis=0),
            jnp.mean(h_mid.astype(jnp.float32), axis=0),
        )
        return out_rows, sample_means

    out_hidden, mean_tuple = lax.map(one_sample, hidden)
    act_mean, head_mean, ln1_mean, ln2_mean = mean_tuple
    f_neuron = jnp.sqrt(jnp.sum(jnp.square(act_mean), axis=0))
    f_head = jnp.sqrt(jnp.sum(jnp.square(head_mean), axis=0))
    f_embed = jnp.sqrt(jnp.sum(jnp.square(ln1_mean), axis=0) + jnp.sum(jnp.square(ln2_mean), axis=0))
    return out_hidden, f_neuron, f_head, f_embed
```

```python
import functools

import jax
import jax.numpy as jnp
from jax import lax
from jax.experimental import pallas as pl
from jax.experimental.pallas import tpu as pltpu
from jax.sharding import PartitionSpec as P

HEAD_DIM = 128
ROT_DIM = 64
ROPE_BASE = 10000.0
LN_EPS = 1e-5
MESH = pl.DeviceIdType.MESH
F32 = jnp.float32
BF16 = jnp.bfloat16

SEQ = 64
ROWS = 128
D = 3072
QL = 1536
KL = 512
FL = 4608
CW = 512
UNIT = 1536
NU = 32
N_O = D // CW
N_UP = FL // CW
N_DN = D // CW
DN_U = FL // UNIT
EH = D + 128

O_U = 10
UP_U = 16
DN_B = 2


def rope_tables(positions):
    half = ROT_DIM // 2
    inv_freq = ROPE_BASE ** (-2.0 * jnp.arange(half, dtype=F32) / ROT_DIM)
    angle = positions.astype(F32)[:, None] * inv_freq[None, :]
    cos, sin = jnp.cos(angle), jnp.sin(angle)
    zero = jnp.zeros_like(sin)
    one = jnp.ones_like(sin)
    keep = jnp.concatenate([cos, cos, one, one], axis=1)
    from_right = jnp.concatenate([-sin, zero, zero, zero], axis=1)
    from_left = jnp.concatenate([zero, sin, zero, zero], axis=1)
    return jnp.stack([keep, from_right, from_left])


def body(sizes, x_hbm, rope_ref, ln_ref, wq, wk, wv, wo, wup, wdn,
         y_hbm, fn_ref, fh_ref, fe_ref,
         wbuf, xb, hb, xm, qs, ks, vs, at, act, osend, orecv, dsend, drecv,
         nsc, esc, are, arn,
         w_sem, d_sem, x_sem, y_sem, tp_send, tp_recv, ar_send, ar_recv):
    dims = sizes
    tp = lax.axis_index("tp")
    dp = lax.axis_index("dp")
    sz, sy, sx = dims
    axes = (
        (lax.rem(dp, sx), sx, 1),
        (lax.rem(lax.div(dp, sx), sy), sy, sx),
        (lax.div(dp, sx * sy), sz, sx * sy),
    )
    partner = 1 - tp

    def peer(axis, k):
        idx, size, stride = axes[axis]
        other = lax.rem(idx + k, size)
        return dp + (other - idx) * stride

    def slot(u, n):
        return wbuf.at[pl.ds(u * UNIT, n * UNIT), :]

    def cols(ref, c):
        return ref.at[:, pl.ds(c * CW, CW)]

    def copy_k():
        return pltpu.make_async_copy(wk, slot(6, 2), w_sem.at[0])

    def copy_v():
        return pltpu.make_async_copy(wv, slot(8, 2), w_sem.at[1])

    def copy_q(c):
        return pltpu.make_async_copy(cols(wq, c), slot(2 * c, 2), w_sem.at[2 + c])

    def copy_o(c):
        return pltpu.make_async_copy(cols(wo, c), slot(O_U + c, 1), w_sem.at[5 + c])

    def up_unit(c):
        return lax.rem(UP_U + 2 * c, NU)

    def copy_up(c):
        return pltpu.make_async_copy(cols(wup, c), slot(up_unit(c), 2), w_sem.at[11 + c])

    def copy_dn(c, u):
        return pltpu.make_async_copy(
            wdn.at[pl.ds(u * UNIT, UNIT), pl.ds(c * CW, CW)],
            slot(DN_B + DN_U * c + u, 1), d_sem.at[DN_U * c + u])

    def start_dn(c):
        for u in range(DN_U):
            copy_dn(c, u).start()

    copy_x = pltpu.make_async_copy(x_hbm, xb, x_sem)
    copy_x.start()
    copy_k().start()
    copy_v().start()
    for c in range(3):
        copy_q(c).start()
    for c in range(N_O):
        copy_o(c).start()
    for c in range(N_UP - 1):
        copy_up(c).start()

    barrier = pltpu.get_barrier_semaphore()
    pl.semaphore_signal(barrier, inc=1, device_id={"tp": partner}, device_id_type=MESH)
    n_peers = 1
    for axis in range(3):
        for k in range(1, axes[axis][1]):
            pl.semaphore_signal(barrier, inc=1, device_id={"dp": peer(axis, k)}, device_id_type=MESH)
            n_peers += 1

    def layer_norm(src, dst, which):
        gain = 1.0 + ln_ref[pl.ds(2 * which, 1), :]
        bias = ln_ref[pl.ds(2 * which + 1, 1), :]
        total = None
        for b in range(ROWS // SEQ):
            def block(i, acc):
                rows = pl.ds(pl.multiple_of(b * SEQ + i * 16, 16), 16)
                v = src[rows, :].astype(F32)
                mean = jnp.mean(v, axis=-1, keepdims=True)
                cen = v - mean
                var = jnp.mean(cen * cen, axis=-1, keepdims=True)
                h = (cen * lax.rsqrt(var + LN_EPS) * gain + bias).astype(BF16)
                dst[rows, :] = h
                return acc + jnp.sum(h.astype(F32), axis=0, keepdims=True)
            acc = lax.fori_loop(0, SEQ // 16, block, jnp.zeros((1, D), F32))
            mean_tok = acc * (1.0 / SEQ)
            sq = mean_tok * mean_tok
            total = sq if total is None else total + sq
        return total

    copy_x.wait()
    esc[:, pl.ds(0, D)] = layer_norm(xb, hb, 0)

    def proj(u):
        return jnp.dot(hb[...], wbuf[pl.ds(u * UNIT, 2 * UNIT), :], preferred_element_type=F32)

    keep = jnp.concatenate([rope_ref[0], rope_ref[0]], axis=0)
    from_right = jnp.concatenate([rope_ref[1], rope_ref[1]], axis=0)
    from_left = jnp.concatenate([rope_ref[2], rope_ref[2]], axis=0)

    def rope(v):
        u = v.astype(BF16).astype(F32)
        r = pltpu.roll(u, HEAD_DIM - ROT_DIM // 2, 1)
        l = pltpu.roll(u, ROT_DIM // 2, 1)
        return (u * keep + r * from_right + l * from_left).astype(BF16)

    copy_k().wait()
    kk = proj(6)
    for g in range(4):
        ks[pl.ds(g * ROWS, ROWS), :] = rope(kk[:, g * HEAD_DIM:(g + 1) * HEAD_DIM])
    copy_v().wait()
    vv = proj(8)
    vs[...] = vv.astype(BF16)

    row = lax.broadcasted_iota(jnp.int32, (3 * ROWS, ROWS), 0) & (ROWS - 1)
    col = lax.broadcasted_iota(jnp.int32, (3 * ROWS, ROWS), 1)
    same = (row >= SEQ) == (col >= SEQ)
    allowed = same & (col <= row)
    blocked = jnp.where(same, F32(-1e30), F32(-jnp.inf))
    lane = lax.broadcasted_iota(jnp.int32, (1, ROWS), 1)

    def attention(g, head_sq):
        q = qs[pl.ds(g * 3 * ROWS, 3 * ROWS), :]
        k = ks[pl.ds(g * ROWS, ROWS), :]
        v = vs[:, g * HEAD_DIM:(g + 1) * HEAD_DIM]
        s = lax.dot_general(q, k, (((1,), (1,)), ((), ())), preferred_element_type=F32) * HEAD_DIM ** -0.5
        s = jnp.where(allowed, s, blocked)
        e = jnp.exp(s - jnp.max(s, axis=-1, keepdims=True))
        p = (e / jnp.sum(e, axis=-1, keepdims=True)).astype(BF16)
        o = jnp.dot(p, v, preferred_element_type=F32).astype(BF16)
        of = o.astype(F32)
        norm = jnp.sqrt(jnp.sum(of * of, axis=-1, keepdims=True))
        for j in range(3):
            i = 3 * g + j
            at[:, i * HEAD_DIM:(i + 1) * HEAD_DIM] = o[j * ROWS:(j + 1) * ROWS, :]
            m0 = jnp.sum(norm[j * ROWS:j * ROWS + SEQ], axis=0, keepdims=True) * (1.0 / SEQ)
            m1 = jnp.sum(norm[j * ROWS + SEQ:(j + 1) * ROWS], axis=0, keepdims=True) * (1.0 / SEQ)
            head_sq = head_sq + jnp.where(lane == i, m0 * m0 + m1 * m1, 0.0)
        return head_sq

    head_sq = jnp.zeros((1, ROWS), F32)
    ready = ((0,), (1,), (2, 3))
    for c in range(3):
        copy_q(c).wait()
        qq = proj(2 * c)
        if c == 0:
            copy_up(N_UP - 1).start()
        for j in range(4):
            qs[pl.ds((4 * c + j) * ROWS, ROWS), :] = rope(qq[:, j * HEAD_DIM:(j + 1) * HEAD_DIM])
        if c == 2:
            start_dn(0)
            start_dn(1)
        for g in ready[c]:
            head_sq = attention(g, head_sq)
    esc[:, pl.ds(D, 128)] = head_sq

    def send_o(c):
        return pltpu.make_async_remote_copy(
            src_ref=osend.at[c], dst_ref=orecv.at[c],
            send_sem=tp_send.at[c], recv_sem=tp_recv.at[c],
            device_id={"tp": partner}, device_id_type=MESH)

    def send_d(c):
        return pltpu.make_async_remote_copy(
            src_ref=dsend.at[c], dst_ref=drecv.at[c],
            send_sem=tp_send.at[N_O + c], recv_sem=tp_recv.at[N_O + c],
            device_id={"tp": partner}, device_id_type=MESH)

    pl.semaphore_wait(barrier, n_peers)

    def finish_o(c):
        send_o(c).wait_recv()
        cs = pl.ds(c * CW, CW)
        xm[:, cs] = (xb[:, cs].astype(F32) + (osend[c] + orecv[c])).astype(BF16)

    for c in range(N_O):
        copy_o(c).wait()
        osend[c] = jnp.dot(at[...], wbuf[pl.ds((O_U + c) * UNIT, UNIT), :], preferred_element_type=F32)
        send_o(c).start()
        if c == 0:
            start_dn(2)
        if c == 3:
            start_dn(3)
        if c >= 1:
            finish_o(c - 1)
    finish_o(N_O - 1)

    esc[:, pl.ds(0, D)] = esc[:, pl.ds(0, D)] + layer_norm(xm, hb, 1)

    def ar_copy(buf, group, axis, k):
        idx = axes[axis][0]
        return pltpu.make_async_remote_copy(
            src_ref=buf.at[axis, idx], dst_ref=buf.at[axis, idx],
            send_sem=ar_send.at[group, axis, k - 1], recv_sem=ar_recv.at[group, axis, k - 1],
            device_id={"dp": peer(axis, k)}, device_id_type=MESH)

    def ar_start(buf, group, axis, value):
        buf[axis, axes[axis][0]] = value
        for k in range(1, axes[axis][1]):
            ar_copy(buf, group, axis, k).start()

    def ar_finish(buf, group, axis):
        for k in range(1, axes[axis][1]):
            ar_copy(buf, group, axis, k).wait()
        total = buf[axis, 0]
        for j in range(1, axes[axis][1]):
            total = total + buf[axis, j]
        return total

    ar_start(are, 0, 0, esc[...])

    def up_chunk(c, _):
        copy_up(c).wait()
        u = jnp.dot(hb[...], wbuf[pl.ds(pl.multiple_of(up_unit(c) * UNIT, UNIT), 2 * UNIT), :],
                    preferred_element_type=F32)
        r = jnp.maximum(u, 0.0)
        a = r * r
        cs = pl.ds(pl.multiple_of(c * CW, CW), CW)
        act[:, cs] = a.astype(BF16)
        m0 = jnp.sum(a[:SEQ], axis=0, keepdims=True) * (1.0 / SEQ)
        m1 = jnp.sum(a[SEQ:], axis=0, keepdims=True) * (1.0 / SEQ)
        nsc[:, cs] = m0 * m0 + m1 * m1
        return 0

    lax.fori_loop(0, 2, up_chunk, 0)
    start_dn(4)
    start_dn(5)
    lax.fori_loop(2, 4, up_chunk, 0)
    ar_start(are, 0, 1, ar_finish(are, 0, 0))
    lax.fori_loop(4, 7, up_chunk, 0)
    ar_start(are, 0, 2, ar_finish(are, 0, 1))
    lax.fori_loop(7, N_UP, up_chunk, 0)
    ar_start(arn, 1, 0, nsc[...])

    def out_copy(c):
        cs = pl.ds(c * CW, CW)
        return pltpu.make_async_copy(xb.at[:, cs], y_hbm.at[:, cs], y_sem.at[c])

    def finish_d(c):
        send_d(c).wait_recv()
        cs = pl.ds(c * CW, CW)
        xb[:, cs] = (xm[:, cs].astype(F32) + (dsend[c] + drecv[c])).astype(BF16)
        out_copy(c).start()

    def down_chunk(c):
        acc = None
        for u in range(DN_U):
            copy_dn(c, u).wait()
            part = jnp.dot(act[:, pl.ds(u * UNIT, UNIT)],
                           wbuf[pl.ds((DN_B + DN_U * c + u) * UNIT, UNIT), :],
                           preferred_element_type=F32)
            acc = part if acc is None else acc + part
        dsend[c] = acc
        send_d(c).start()

    def finish_e():
        total = jnp.sqrt(ar_finish(are, 0, 2))
        fe_ref[...] = total[:, :D]
        fh_ref[...] = total[:, D:]

    for c in range(N_DN):
        down_chunk(c)
        if c >= 1:
            finish_d(c - 1)
        if c == 1:
            finish_e()
            ar_start(arn, 1, 1, ar_finish(arn, 1, 0))
        if c == 4:
            ar_start(arn, 1, 2, ar_finish(arn, 1, 1))
    finish_d(N_DN - 1)
    fn_ref[...] = jnp.sqrt(ar_finish(arn, 1, 2))

    for c in range(N_O):
        send_o(c).wait_send()
    for c in range(N_DN):
        send_d(c).wait_send()
        out_copy(c).wait()


def solution(mesh):
    dims = (4, 4, 4)

    def local_layer(hidden, positions, ln1_gain, ln1_bias, w_q, w_k, w_v, w_o, ln2_gain, ln2_bias, w_up, w_down):
        ln = jnp.stack([ln1_gain, ln1_bias, ln2_gain, ln2_bias]).astype(F32)
        rope = rope_tables(positions)
        any_spec = pl.BlockSpec(memory_space=pltpu.HBM)
        vmem = pl.BlockSpec(memory_space=pltpu.VMEM)
        y, fn, fh, fe = pl.pallas_call(
            functools.partial(body, dims),
            out_shape=(
                jax.ShapeDtypeStruct((ROWS, D), BF16),
                jax.ShapeDtypeStruct((1, FL), F32),
                jax.ShapeDtypeStruct((1, 128), F32),
                jax.ShapeDtypeStruct((1, D), F32),
            ),
            in_specs=[any_spec, vmem, vmem] + [any_spec] * 6,
            out_specs=(any_spec, vmem, vmem, vmem),
            scratch_shapes=[
                pltpu.VMEM((NU * UNIT, CW), BF16),
                pltpu.VMEM((ROWS, D), BF16),
                pltpu.VMEM((ROWS, D), BF16),
                pltpu.VMEM((ROWS, D), BF16),
                pltpu.VMEM((12 * ROWS, HEAD_DIM), BF16),
                pltpu.VMEM((4 * ROWS, HEAD_DIM), BF16),
                pltpu.VMEM((ROWS, KL), BF16),
                pltpu.VMEM((ROWS, QL), BF16),
                pltpu.VMEM((ROWS, FL), BF16),
                pltpu.VMEM((N_O, ROWS, CW), F32),
                pltpu.VMEM((N_O, ROWS, CW), F32),
                pltpu.VMEM((N_DN, ROWS, CW), F32),
                pltpu.VMEM((N_DN, ROWS, CW), F32),
                pltpu.VMEM((1, FL), F32),
                pltpu.VMEM((1, EH), F32),
                pltpu.VMEM((3, 4, 1, EH), F32),
                pltpu.VMEM((3, 4, 1, FL), F32),
                pltpu.SemaphoreType.DMA((20,)),
                pltpu.SemaphoreType.DMA((N_DN * DN_U,)),
                pltpu.SemaphoreType.DMA,
                pltpu.SemaphoreType.DMA((N_DN,)),
                pltpu.SemaphoreType.DMA((N_O + N_DN,)),
                pltpu.SemaphoreType.DMA((N_O + N_DN,)),
                pltpu.SemaphoreType.DMA((2, 3, 3)),
                pltpu.SemaphoreType.DMA((2, 3, 3)),
            ],
            compiler_params=pltpu.CompilerParams(
                collective_id=0, has_side_effects=True, vmem_limit_bytes=67043328),
            name="layer",
        )(hidden.reshape(ROWS, D), rope, ln, w_q, w_k, w_v, w_o, w_up, w_down)
        return y.reshape(hidden.shape), fn.reshape(FL), fh[0, :12], fe.reshape(D)

    weight_col = P(None, "tp")
    weight_row = P("tp", None)
    return jax.shard_map(
        local_layer,
        mesh=mesh,
        in_specs=(P("dp"), P(), P(), P(), weight_col, weight_col, weight_col, weight_row, P(), P(), weight_col, weight_row),
        out_specs=(P("dp"), P("tp"), P("tp"), P()),
        check_vma=False,
    )
```

```python
import functools

import jax
import jax.numpy as jnp
import numpy as np
from jax import lax
from jax.experimental import pallas as pl
from jax.experimental.pallas import tpu as pltpu
from jax.sharding import PartitionSpec as P

HEAD_DIM = 128
ROT_DIM = 64
ROPE_BASE = 10000.0
LN_EPS = 1e-5
MESH = pl.DeviceIdType.MESH
F32 = jnp.float32
BF16 = jnp.bfloat16

SEQ = 64
ROWS = 128
D = 3072
QL = 1536
KL = 512
FL = 4608
CW = 512
UNIT = 1536
NU = 32
N_O = D // CW
N_UP = FL // CW
PN = FL // 3
N_DN = D // CW
DN_U = FL // UNIT
EH = D + 128

O_U = 10
UP_U = 16
DN_B = 2


def inv_freq_row():
    half = ROT_DIM // 2
    freq = ROPE_BASE ** (-2.0 * np.arange(half, dtype=np.float64) / ROT_DIM)
    return np.concatenate([freq, freq, np.zeros(HEAD_DIM - ROT_DIM)])[None, :].astype(np.float32)


def body(sizes, x_hbm, pos_hbm, freq_hbm, g1, b1, g2, b2, wq, wk, wv, wo, wup, wdn,
         y_ref, fn_ref, fh_ref, fe_ref,
         wbuf, ln0, ln1, ln2, ln3, posb, freqb, xb, hb, xm, qs, ks, vs, at, act, osend, orecv, dsend, drecv,
         nsc, esc, are, arn,
         w_sem, d_sem, x_sem, tp_send, tp_recv, ar_send, ar_recv):
    dims = sizes
    tp = lax.axis_index("tp")
    dp = lax.axis_index("dp")
    sz, sy, sx = dims
    axes = (
        (lax.rem(dp, sx), sx, 1),
        (lax.rem(lax.div(dp, sx), sy), sy, sx),
        (lax.div(dp, sx * sy), sz, sx * sy),
    )
    partner = 1 - tp

    def peer(axis, k):
        idx, size, stride = axes[axis]
        other = lax.rem(idx + k, size)
        return dp + (other - idx) * stride

    def slot(u, n):
        return wbuf.at[pl.ds(u * UNIT, n * UNIT), :]

    def cols(ref, c):
        return ref.at[:, pl.ds(c * CW, CW)]

    def copy_k():
        return pltpu.make_async_copy(wk, slot(6, 2), w_sem.at[0])

    def copy_v():
        return pltpu.make_async_copy(wv, slot(8, 2), w_sem.at[1])

    def copy_q(c):
        return pltpu.make_async_copy(cols(wq, c), slot(2 * c, 2), w_sem.at[2 + c])

    def copy_o(c):
        return pltpu.make_async_copy(cols(wo, c), slot(O_U + c, 1), w_sem.at[5 + c])

    def up_unit(c):
        return lax.rem(UP_U + 2 * c, NU)

    def copy_up(c):
        return pltpu.make_async_copy(cols(wup, c), slot(up_unit(c), 2), w_sem.at[11 + c])

    def copy_dn(c, u):
        return pltpu.make_async_copy(
            wdn.at[pl.ds(u * UNIT, UNIT), pl.ds(c * CW, CW)],
            slot(DN_B + DN_U * c + u, 1), d_sem.at[DN_U * c + u])

    def start_dn(c):
        for u in range(DN_U):
            copy_dn(c, u).start()

    def copy_x():
        return pltpu.make_async_copy(x_hbm, xb, x_sem.at[0])

    lnb = (ln0, ln1, ln2, ln3)
    small = [pltpu.make_async_copy(r, lnb[i], x_sem.at[1 + i]) for i, r in enumerate((g1, b1, g2, b2))]
    small.append(pltpu.make_async_copy(pos_hbm, posb, x_sem.at[5]))
    small.append(pltpu.make_async_copy(freq_hbm, freqb, x_sem.at[6]))

    barrier = pltpu.get_barrier_semaphore()
    greet = [{"tp": partner}]
    for axis in range(3):
        for k in range(1, axes[axis][1]):
            greet.append({"dp": peer(axis, k)})
    first = [lambda: [copy_x().start()], lambda: [c.start() for c in small],
             lambda: [copy_k().start()], lambda: [copy_v().start()]]
    first += [lambda c=c: [copy_q(c).start()] for c in range(3)]
    first += [lambda c=c: [copy_o(c).start()] for c in range(N_O)]
    for i in range(max(len(first), len(greet))):
        if i < len(first):
            first[i]()
        if i < len(greet):
            pl.semaphore_signal(barrier, inc=1, device_id=greet[i], device_id_type=MESH)
    n_peers = len(greet)

    def layer_norm(src, dst, which):
        gain = 1.0 + lnb[2 * which][...].astype(F32).reshape(1, D)
        bias = lnb[2 * which + 1][...].astype(F32).reshape(1, D)
        total = None
        for b in range(ROWS // SEQ):
            def block(i, acc):
                rows = pl.ds(pl.multiple_of(b * SEQ + i * 16, 16), 16)
                v = src[rows, :].astype(F32)
                mean = jnp.mean(v, axis=-1, keepdims=True)
                cen = v - mean
                var = jnp.mean(cen * cen, axis=-1, keepdims=True)
                h = (cen * lax.rsqrt(var + LN_EPS) * gain + bias).astype(BF16)
                dst[rows, :] = h
                return acc + jnp.sum(h.astype(F32), axis=0, keepdims=True)
            acc = lax.fori_loop(0, SEQ // 16, block, jnp.zeros((1, D), F32))
            mean_tok = acc * (1.0 / SEQ)
            sq = mean_tok * mean_tok
            total = sq if total is None else total + sq
        return total

    for c in small:
        c.wait()
    diag = (lax.broadcasted_iota(jnp.int32, (SEQ, SEQ), 0)
            == lax.broadcasted_iota(jnp.int32, (SEQ, SEQ), 1))
    pos_row = jnp.broadcast_to(posb[...].astype(F32).reshape(1, SEQ), (SEQ, SEQ))
    pos_col = jnp.sum(jnp.where(diag, pos_row, 0.0), axis=1, keepdims=True)
    angle = pos_col * freqb[...]
    cos, sin = jnp.cos(angle), jnp.sin(angle)
    hl = lax.broadcasted_iota(jnp.int32, (SEQ, HEAD_DIM), 1)
    keep = jnp.where(hl < ROT_DIM, cos, 1.0)
    from_right = jnp.where(hl < ROT_DIM // 2, -sin, 0.0)
    from_left = jnp.where((hl >= ROT_DIM // 2) & (hl < ROT_DIM), sin, 0.0)
    keep = jnp.concatenate([keep, keep], axis=0)
    from_right = jnp.concatenate([from_right, from_right], axis=0)
    from_left = jnp.concatenate([from_left, from_left], axis=0)

    copy_x().wait()
    copy_up(0).start()
    copy_up(1).start()
    esc[:, pl.ds(0, D)] = layer_norm(xb, hb, 0)

    def proj(u):
        return jnp.dot(hb[...], wbuf[pl.ds(u * UNIT, 2 * UNIT), :], preferred_element_type=F32)

    def rope(v):
        u = v.astype(BF16).astype(F32)
        r = pltpu.roll(u, HEAD_DIM - ROT_DIM // 2, 1)
        l = pltpu.roll(u, ROT_DIM // 2, 1)
        return (u * keep + r * from_right + l * from_left).astype(BF16)

    copy_k().wait()
    copy_up(2).start()
    copy_up(3).start()
    kk = proj(6)
    for g in range(4):
        ks[pl.ds(g * ROWS, ROWS), :] = rope(kk[:, g * HEAD_DIM:(g + 1) * HEAD_DIM])
    copy_v().wait()
    copy_up(4).start()
    copy_up(5).start()
    vv = proj(8)
    vs[...] = vv.astype(BF16)

    row = lax.broadcasted_iota(jnp.int32, (3 * ROWS, ROWS), 0) & (ROWS - 1)
    col = lax.broadcasted_iota(jnp.int32, (3 * ROWS, ROWS), 1)
    same = (row >= SEQ) == (col >= SEQ)
    allowed = same & (col <= row)
    blocked = jnp.where(same, F32(-1e30), F32(-jnp.inf))
    lane = lax.broadcasted_iota(jnp.int32, (1, ROWS), 1)

    def attention(g, head_sq):
        q = qs[pl.ds(g * 3 * ROWS, 3 * ROWS), :]
        k = ks[pl.ds(g * ROWS, ROWS), :]
        v = vs[:, g * HEAD_DIM:(g + 1) * HEAD_DIM]
        s = lax.dot_general(q, k, (((1,), (1,)), ((), ())), preferred_element_type=F32) * HEAD_DIM ** -0.5
        s = jnp.where(allowed, s, blocked)
        e = jnp.exp(s - jnp.max(s, axis=-1, keepdims=True))
        p = (e / jnp.sum(e, axis=-1, keepdims=True)).astype(BF16)
        o = jnp.dot(p, v, preferred_element_type=F32).astype(BF16)
        of = o.astype(F32)
        norm = jnp.sqrt(jnp.sum(of * of, axis=-1, keepdims=True))
        for j in range(3):
            i = 3 * g + j
            at[:, i * HEAD_DIM:(i + 1) * HEAD_DIM] = o[j * ROWS:(j + 1) * ROWS, :]
            m0 = jnp.sum(norm[j * ROWS:j * ROWS + SEQ], axis=0, keepdims=True) * (1.0 / SEQ)
            m1 = jnp.sum(norm[j * ROWS + SEQ:(j + 1) * ROWS], axis=0, keepdims=True) * (1.0 / SEQ)
            head_sq = head_sq + jnp.where(lane == i, m0 * m0 + m1 * m1, 0.0)
        return head_sq

    head_sq = jnp.zeros((1, ROWS), F32)
    ready = ((0,), (1,), (2, 3))
    for c in range(3):
        copy_q(c).wait()
        if c == 0:
            copy_up(6).start()
            copy_up(7).start()
        qq = proj(2 * c)
        if c == 0:
            copy_up(N_UP - 1).start()
        for j in range(4):
            qs[pl.ds((4 * c + j) * ROWS, ROWS), :] = rope(qq[:, j * HEAD_DIM:(j + 1) * HEAD_DIM])
        if c == 2:
            start_dn(0)
            start_dn(1)
        for g in ready[c]:
            head_sq = attention(g, head_sq)
    esc[:, pl.ds(D, 128)] = head_sq

    def send_o(c):
        return pltpu.make_async_remote_copy(
            src_ref=osend.at[c], dst_ref=orecv.at[c],
            send_sem=tp_send.at[c], recv_sem=tp_recv.at[c],
            device_id={"tp": partner}, device_id_type=MESH)

    def send_d(c):
        return pltpu.make_async_remote_copy(
            src_ref=dsend.at[c], dst_ref=drecv.at[c],
            send_sem=tp_send.at[N_O + c], recv_sem=tp_recv.at[N_O + c],
            device_id={"tp": partner}, device_id_type=MESH)

    pl.semaphore_wait(barrier, n_peers)

    def finish_o(c):
        send_o(c).wait_recv()
        cs = pl.ds(c * CW, CW)
        xm[:, cs] = (xb[:, cs].astype(F32) + (osend[c] + orecv[c])).astype(BF16)

    for c in range(N_O):
        copy_o(c).wait()
        osend[c] = jnp.dot(at[...], wbuf[pl.ds((O_U + c) * UNIT, UNIT), :], preferred_element_type=F32)
        send_o(c).start()
        if c == 0:
            start_dn(2)
        if c == 3:
            start_dn(3)
        if c >= 1:
            finish_o(c - 1)
    finish_o(N_O - 1)

    esc[:, pl.ds(0, D)] = esc[:, pl.ds(0, D)] + layer_norm(xm, hb, 1)

    def ar_copy(buf, group, phase, axis, k):
        idx = axes[axis][0]
        return pltpu.make_async_remote_copy(
            src_ref=buf.at[phase, idx], dst_ref=buf.at[phase, idx],
            send_sem=ar_send.at[group, phase, k - 1], recv_sem=ar_recv.at[group, phase, k - 1],
            device_id={"dp": peer(axis, k)}, device_id_type=MESH)

    def ar_start(buf, group, phase, axis, value):
        buf[phase, axes[axis][0]] = value
        for k in range(1, axes[axis][1]):
            ar_copy(buf, group, phase, axis, k).start()

    def ar_finish(buf, group, phase, axis):
        for k in range(1, axes[axis][1]):
            ar_copy(buf, group, phase, axis, k).wait()
        total = buf[phase, 0]
        for j in range(1, axes[axis][1]):
            total = total + buf[phase, j]
        return total

    def e_start(phase, value):
        ar_start(are, 3, phase, phase, value)

    def e_finish(phase):
        return ar_finish(are, 3, phase, phase)

    def n_step(phase):
        for part in range(3):
            if phase == 0:
                value = nsc[:, pl.ds(part * PN, PN)]
            else:
                value = ar_finish(arn.at[part], part, phase - 1, (part + phase - 1) % 3)
            if phase < 3:
                ar_start(arn.at[part], part, phase, (part + phase) % 3, value)
            else:
                fn_ref[pl.ds(part * PN, PN)] = jnp.sqrt(value).reshape(PN)

    e_start(0, esc[...])

    def up_chunk(c, _):
        copy_up(c).wait()
        u = jnp.dot(hb[...], wbuf[pl.ds(pl.multiple_of(up_unit(c) * UNIT, UNIT), 2 * UNIT), :],
                    preferred_element_type=F32)
        r = jnp.maximum(u, 0.0)
        a = r * r
        cs = pl.ds(pl.multiple_of(c * CW, CW), CW)
        act[:, cs] = a.astype(BF16)
        m0 = jnp.sum(a[:SEQ], axis=0, keepdims=True) * (1.0 / SEQ)
        m1 = jnp.sum(a[SEQ:], axis=0, keepdims=True) * (1.0 / SEQ)
        nsc[:, cs] = m0 * m0 + m1 * m1
        return 0

    lax.fori_loop(0, 2, up_chunk, 0)
    start_dn(4)
    lax.fori_loop(2, 4, up_chunk, 0)
    copy_dn(5, 0).start()
    lax.fori_loop(4, 6, up_chunk, 0)
    copy_dn(5, 1).start()
    lax.fori_loop(6, N_UP, up_chunk, 0)
    n_step(0)
    copy_dn(5, 2).start()
    e_start(1, e_finish(0))

    def finish_d(c):
        send_d(c).wait_recv()
        cs = pl.ds(c * CW, CW)
        y_ref[:, cs] = (xm[:, cs].astype(F32) + (dsend[c] + drecv[c])).astype(BF16)

    def finish_e():
        total = jnp.sqrt(e_finish(2))
        fe_ref[...] = total[:, :D].reshape(D)
        fh_ref[...] = total[:, D:].reshape(128)[:12]

    hooks = {
        (1, 2): lambda: e_start(2, e_finish(1)),
        (2, 1): lambda: n_step(1),
        (3, 2): finish_e,
        (4, 2): lambda: n_step(2),
    }

    for c in range(N_DN):
        acc = None
        for u in range(DN_U):
            copy_dn(c, u).wait()
            part = jnp.dot(act[:, pl.ds(u * UNIT, UNIT)],
                           wbuf[pl.ds((DN_B + DN_U * c + u) * UNIT, UNIT), :],
                           preferred_element_type=F32)
            acc = part if acc is None else acc + part
            if u == DN_U - 1:
                dsend[c] = acc
                send_d(c).start()
            if (c, u) in hooks:
                hooks[c, u]()
        if c >= 1:
            finish_d(c - 1)
    finish_d(N_DN - 1)
    n_step(3)

    for c in range(N_O):
        send_o(c).wait_send()
    for c in range(N_DN):
        send_d(c).wait_send()


def solution(mesh):
    dims = (4, 4, 4)

    def local_layer(hidden, positions, ln1_gain, ln1_bias, w_q, w_k, w_v, w_o, ln2_gain, ln2_bias, w_up, w_down):
        hbm = pl.BlockSpec(memory_space=pltpu.HBM)
        vmem = pl.BlockSpec(memory_space=pltpu.VMEM)
        y, fn, fh, fe = pl.pallas_call(
            functools.partial(body, dims),
            out_shape=(
                pltpu.VMEM((ROWS, D), BF16),
                pltpu.VMEM((FL,), F32),
                pltpu.VMEM((12,), F32),
                pltpu.VMEM((D,), F32),
            ),
            in_specs=[hbm] * 13,
            out_specs=(vmem, vmem, vmem, vmem),
            scratch_shapes=[
                pltpu.VMEM((NU * UNIT, CW), BF16),
                pltpu.VMEM((D,), BF16),
                pltpu.VMEM((D,), BF16),
                pltpu.VMEM((D,), BF16),
                pltpu.VMEM((D,), BF16),
                pltpu.VMEM((SEQ,), jnp.int32),
                pltpu.VMEM((1, HEAD_DIM), F32),
                pltpu.VMEM((ROWS, D), BF16),
                pltpu.VMEM((ROWS, D), BF16),
                pltpu.VMEM((ROWS, D), BF16),
                pltpu.VMEM((12 * ROWS, HEAD_DIM), BF16),
                pltpu.VMEM((4 * ROWS, HEAD_DIM), BF16),
                pltpu.VMEM((ROWS, KL), BF16),
                pltpu.VMEM((ROWS, QL), BF16),
                pltpu.VMEM((ROWS, FL), BF16),
                pltpu.VMEM((N_O, ROWS, CW), F32),
                pltpu.VMEM((N_O, ROWS, CW), F32),
                pltpu.VMEM((N_DN, ROWS, CW), F32),
                pltpu.VMEM((N_DN, ROWS, CW), F32),
                pltpu.VMEM((1, FL), F32),
                pltpu.VMEM((1, EH), F32),
                pltpu.VMEM((3, 4, 1, EH), F32),
                pltpu.VMEM((3, 3, 4, 1, PN), F32),
                pltpu.SemaphoreType.DMA((20,)),
                pltpu.SemaphoreType.DMA((N_DN * DN_U,)),
                pltpu.SemaphoreType.DMA((7,)),
                pltpu.SemaphoreType.DMA((N_O + N_DN,)),
                pltpu.SemaphoreType.DMA((N_O + N_DN,)),
                pltpu.SemaphoreType.DMA((4, 3, 3)),
                pltpu.SemaphoreType.DMA((4, 3, 3)),
            ],
            compiler_params=pltpu.CompilerParams(
                collective_id=0, has_side_effects=True, vmem_limit_bytes=62 * 2**20),
            name="layer",
        )(hidden.reshape(ROWS, D), positions, jnp.asarray(inv_freq_row()), ln1_gain, ln1_bias, ln2_gain, ln2_bias,
          w_q, w_k, w_v, w_o, w_up, w_down)
        return y.reshape(hidden.shape), fn, fh, fe

    weight_col = P(None, "tp")
    weight_row = P("tp", None)
    return jax.shard_map(
        local_layer,
        mesh=mesh,
        in_specs=(P("dp"), P(), P(), P(), weight_col, weight_col, weight_col, weight_row, P(), P(), weight_col, weight_row),
        out_specs=(P("dp"), P("tp"), P("tp"), P()),
        check_vma=False,
    )
```

```python
import functools

import jax
import jax.numpy as jnp
import numpy as np
from jax import lax
from jax.experimental import pallas as pl
from jax.experimental.pallas import tpu as pltpu
from jax.sharding import PartitionSpec as P

HEAD_DIM = 128
ROT_DIM = 64
ROPE_BASE = 10000.0
LN_EPS = 1e-5
MESH = pl.DeviceIdType.MESH
F32 = jnp.float32
BF16 = jnp.bfloat16

SEQ = 64
ROWS = 128
D = 3072
QL = 1536
KL = 512
FL = 4608
CW = 512
UNIT = 1536
NU = 32
N_O = D // CW
N_UP = FL // CW
PN = FL // 3
N_DN = D // CW
DN_U = FL // UNIT
EH = D + 128

O_U = 10
UP_U = 16
DN_B = 2


def inv_freq_row():
    half = ROT_DIM // 2
    freq = ROPE_BASE ** (-2.0 * np.arange(half, dtype=np.float64) / ROT_DIM)
    return np.concatenate([freq, freq, np.zeros(HEAD_DIM - ROT_DIM)])[None, :].astype(np.float32)


def body(sizes, x_hbm, pos_hbm, freq_hbm, g1, b1, g2, b2, wq, wk, wv, wo, wup, wdn,
         y_ref, fn_ref, fh_ref, fe_ref,
         wbuf, ln0, ln1, ln2, ln3, posb, freqb, xb, hb, xm, qs, ks, vs, at, act, osend, orecv, dsend, drecv,
         nsc, esc, are, arn,
         w_sem, d_sem, x_sem, tp_send, tp_recv, ar_send, ar_recv):
    dims = sizes
    tp = lax.axis_index("tp")
    dp = lax.axis_index("dp")
    sz, sy, sx = dims
    axes = (
        (lax.rem(dp, sx), sx, 1),
        (lax.rem(lax.div(dp, sx), sy), sy, sx),
        (lax.div(dp, sx * sy), sz, sx * sy),
    )
    partner = 1 - tp

    def peer(axis, k):
        idx, size, stride = axes[axis]
        other = lax.rem(idx + k, size)
        return dp + (other - idx) * stride

    def slot(u, n):
        return wbuf.at[pl.ds(u * UNIT, n * UNIT), :]

    def cols(ref, c):
        return ref.at[:, pl.ds(c * CW, CW)]

    def copy_k():
        return pltpu.make_async_copy(wk, slot(6, 2), w_sem.at[0])

    def copy_v():
        return pltpu.make_async_copy(wv, slot(8, 2), w_sem.at[1])

    def copy_q(c):
        return pltpu.make_async_copy(cols(wq, c), slot(2 * c, 2), w_sem.at[2 + c])

    def copy_o(c):
        return pltpu.make_async_copy(cols(wo, c), slot(O_U + c, 1), w_sem.at[5 + c])

    def up_unit(c):
        return lax.rem(UP_U + 2 * c, NU)

    def copy_up(c):
        return pltpu.make_async_copy(cols(wup, c), slot(up_unit(c), 2), w_sem.at[11 + c])

    def copy_dn(c, u=0, n=DN_U):
        return pltpu.make_async_copy(
            wdn.at[pl.ds(u * UNIT, n * UNIT), pl.ds(c * CW, CW)],
            slot(DN_B + DN_U * c + u, n), d_sem.at[c + u])

    def copy_x():
        return pltpu.make_async_copy(x_hbm, xb, x_sem.at[0])

    lnb = (ln0, ln1, ln2, ln3)
    small = [pltpu.make_async_copy(r, lnb[i], x_sem.at[1 + i]) for i, r in enumerate((g1, b1, g2, b2))]
    small.append(pltpu.make_async_copy(pos_hbm, posb, x_sem.at[5]))
    small.append(pltpu.make_async_copy(freq_hbm, freqb, x_sem.at[6]))

    barrier = pltpu.get_barrier_semaphore()
    greet = [{"tp": partner}]
    for axis in range(3):
        for k in range(1, axes[axis][1]):
            greet.append({"dp": peer(axis, k)})
    first = [lambda: [copy_x().start()], lambda: [c.start() for c in small],
             lambda: [copy_k().start()], lambda: [copy_v().start()]]
    first += [lambda c=c: [copy_q(c).start()] for c in range(3)]
    first += [lambda c=c: [copy_o(c).start()] for c in range(N_O)]
    for i in range(max(len(first), len(greet))):
        if i < len(first):
            first[i]()
        if i < len(greet):
            pl.semaphore_signal(barrier, inc=1, device_id=greet[i], device_id_type=MESH)
    n_peers = len(greet)

    def layer_norm(src, dst, which):
        gain = 1.0 + lnb[2 * which][...].astype(F32).reshape(1, D)
        bias = lnb[2 * which + 1][...].astype(F32).reshape(1, D)
        total = None
        for b in range(ROWS // SEQ):
            acc = None
            for i in range(SEQ // 16):
                rows = pl.ds(b * SEQ + i * 16, 16)
                v = src[rows, :].astype(F32)
                mean = jnp.mean(v, axis=-1, keepdims=True)
                cen = v - mean
                var = jnp.mean(cen * cen, axis=-1, keepdims=True)
                h = (cen * lax.rsqrt(var + LN_EPS) * gain + bias).astype(BF16)
                dst[rows, :] = h
                hf = h.astype(F32)
                part = hf[:8] + hf[8:]
                acc = part if acc is None else acc + part
            mean_tok = jnp.sum(acc, axis=0, keepdims=True) * (1.0 / SEQ)
            sq = mean_tok * mean_tok
            total = sq if total is None else total + sq
        return total

    for c in small:
        c.wait()
    copy_x().wait()
    copy_up(0).start()
    copy_up(1).start()
    esc[:, pl.ds(0, D)] = layer_norm(xb, hb, 0)

    diag = (lax.broadcasted_iota(jnp.int32, (SEQ, SEQ), 0)
            == lax.broadcasted_iota(jnp.int32, (SEQ, SEQ), 1))
    pos_row = jnp.broadcast_to(posb[...].astype(F32).reshape(1, SEQ), (SEQ, SEQ))
    pos_col = jnp.sum(jnp.where(diag, pos_row, 0.0), axis=1, keepdims=True)
    angle = pos_col * freqb[...]
    cos, sin = jnp.cos(angle), jnp.sin(angle)
    hl = lax.broadcasted_iota(jnp.int32, (SEQ, HEAD_DIM), 1)
    keep = jnp.where(hl < ROT_DIM, cos, 1.0)
    from_right = jnp.where(hl < ROT_DIM // 2, -sin, 0.0)
    from_left = jnp.where((hl >= ROT_DIM // 2) & (hl < ROT_DIM), sin, 0.0)
    keep = jnp.concatenate([keep, keep], axis=0)
    from_right = jnp.concatenate([from_right, from_right], axis=0)
    from_left = jnp.concatenate([from_left, from_left], axis=0)

    def proj(u):
        return jnp.dot(hb[...], wbuf[pl.ds(u * UNIT, 2 * UNIT), :], preferred_element_type=F32)

    def rope(v):
        u = v.astype(BF16).astype(F32)
        r = pltpu.roll(u, HEAD_DIM - ROT_DIM // 2, 1)
        l = pltpu.roll(u, ROT_DIM // 2, 1)
        return (u * keep + r * from_right + l * from_left).astype(BF16)

    copy_k().wait()
    copy_up(2).start()
    copy_up(3).start()
    copy_v().wait()
    copy_up(4).start()
    copy_up(5).start()
    kk = proj(6)
    vv = proj(8)
    for g in range(4):
        ks[pl.ds(g * ROWS, ROWS), :] = rope(kk[:, g * HEAD_DIM:(g + 1) * HEAD_DIM])
    vs[...] = vv.astype(BF16)

    row = lax.broadcasted_iota(jnp.int32, (3 * ROWS, ROWS), 0) & (ROWS - 1)
    col = lax.broadcasted_iota(jnp.int32, (3 * ROWS, ROWS), 1)
    same = (row >= SEQ) == (col >= SEQ)
    allowed = same & (col <= row)
    blocked = jnp.where(same, F32(-1e30), F32(-jnp.inf))
    lane = lax.broadcasted_iota(jnp.int32, (1, ROWS), 1)

    def attention(g, head_sq):
        q = qs[pl.ds(g * 3 * ROWS, 3 * ROWS), :]
        k = ks[pl.ds(g * ROWS, ROWS), :]
        v = vs[:, g * HEAD_DIM:(g + 1) * HEAD_DIM]
        s = lax.dot_general(q, k, (((1,), (1,)), ((), ())), preferred_element_type=F32) * HEAD_DIM ** -0.5
        s = jnp.where(allowed, s, blocked)
        e = jnp.exp(s - jnp.max(s, axis=-1, keepdims=True))
        p = (e / jnp.sum(e, axis=-1, keepdims=True)).astype(BF16)
        o = jnp.dot(p, v, preferred_element_type=F32).astype(BF16)
        of = o.astype(F32)
        norm = jnp.sqrt(jnp.sum(of * of, axis=-1, keepdims=True))
        for j in range(3):
            i = 3 * g + j
            at[:, i * HEAD_DIM:(i + 1) * HEAD_DIM] = o[j * ROWS:(j + 1) * ROWS, :]
            m0 = jnp.sum(norm[j * ROWS:j * ROWS + SEQ], axis=0, keepdims=True) * (1.0 / SEQ)
            m1 = jnp.sum(norm[j * ROWS + SEQ:(j + 1) * ROWS], axis=0, keepdims=True) * (1.0 / SEQ)
            head_sq = head_sq + jnp.where(lane == i, m0 * m0 + m1 * m1, 0.0)
        return head_sq

    def query(c):
        qq = proj(2 * c)
        for j in range(4):
            qs[pl.ds((4 * c + j) * ROWS, ROWS), :] = rope(qq[:, j * HEAD_DIM:(j + 1) * HEAD_DIM])

    head_sq = jnp.zeros((1, ROWS), F32)
    copy_q(0).wait()
    copy_up(6).start()
    copy_up(7).start()
    copy_q(1).wait()
    query(0)
    query(1)
    head_sq = attention(0, head_sq)
    head_sq = attention(1, head_sq)
    copy_q(2).wait()
    copy_up(N_UP - 1).start()
    query(2)
    head_sq = attention(2, head_sq)
    head_sq = attention(3, head_sq)
    esc[:, pl.ds(D, 128)] = head_sq

    def send_o(c):
        return pltpu.make_async_remote_copy(
            src_ref=osend.at[c], dst_ref=orecv.at[c],
            send_sem=tp_send.at[c], recv_sem=tp_recv.at[c],
            device_id={"tp": partner}, device_id_type=MESH)

    def send_d(c):
        return pltpu.make_async_remote_copy(
            src_ref=dsend.at[c], dst_ref=drecv.at[c],
            send_sem=tp_send.at[N_O + c], recv_sem=tp_recv.at[N_O + c],
            device_id={"tp": partner}, device_id_type=MESH)

    pl.semaphore_wait(barrier, n_peers)

    def finish_o(c):
        send_o(c).wait_recv()
        cs = pl.ds(c * CW, CW)
        xm[:, cs] = (xb[:, cs].astype(F32) + (osend[c] + orecv[c])).astype(BF16)

    for part in range(2):
        for c in range(3 * part, 3 * part + 3):
            copy_o(c).wait()
        if part == 0:
            copy_dn(0).start()
            copy_dn(1).start()
        else:
            copy_dn(2).start()
        for c in range(3 * part, 3 * part + 3):
            osend[c] = jnp.dot(at[...], wbuf[pl.ds((O_U + c) * UNIT, UNIT), :], preferred_element_type=F32)
            send_o(c).start()
        if part == 1:
            copy_dn(3).start()
    for c in range(N_O):
        finish_o(c)

    esc[:, pl.ds(0, D)] = esc[:, pl.ds(0, D)] + layer_norm(xm, hb, 1)

    def ar_copy(buf, group, phase, axis, k):
        idx = axes[axis][0]
        return pltpu.make_async_remote_copy(
            src_ref=buf.at[phase, idx], dst_ref=buf.at[phase, idx],
            send_sem=ar_send.at[group, phase, k - 1], recv_sem=ar_recv.at[group, phase, k - 1],
            device_id={"dp": peer(axis, k)}, device_id_type=MESH)

    def ar_start(buf, group, phase, axis, value):
        buf[phase, axes[axis][0]] = value
        for k in range(1, axes[axis][1]):
            ar_copy(buf, group, phase, axis, k).start()

    def ar_finish(buf, group, phase, axis):
        for k in range(1, axes[axis][1]):
            ar_copy(buf, group, phase, axis, k).wait()
        total = buf[phase, 0]
        for j in range(1, axes[axis][1]):
            total = total + buf[phase, j]
        return total

    def e_start(phase, value):
        ar_start(are, 3, phase, phase, value)

    def e_finish(phase):
        return ar_finish(are, 3, phase, phase)

    def n_step(phase):
        for part in range(3):
            if phase == 0:
                value = nsc[:, pl.ds(part * PN, PN)]
            else:
                value = ar_finish(arn.at[part], part, phase - 1, (part + phase - 1) % 3)
            if phase < 3:
                ar_start(arn.at[part], part, phase, (part + phase) % 3, value)
            else:
                fn_ref[pl.ds(part * PN, PN)] = jnp.sqrt(value).reshape(PN)

    e_start(0, esc[...])

    def up_chunk(c):
        u = jnp.dot(hb[...], wbuf[pl.ds((UP_U + 2 * c) % NU * UNIT, 2 * UNIT), :], preferred_element_type=F32)
        r = jnp.maximum(u, 0.0)
        a = r * r
        cs = pl.ds(c * CW, CW)
        act[:, cs] = a.astype(BF16)
        m0 = jnp.sum(a[:SEQ], axis=0, keepdims=True) * (1.0 / SEQ)
        m1 = jnp.sum(a[SEQ:], axis=0, keepdims=True) * (1.0 / SEQ)
        nsc[:, cs] = m0 * m0 + m1 * m1

    for i, chunks in enumerate(((0, 1, 2), (3, 4, 5), (6, 7), (8,))):
        for c in chunks:
            copy_up(c).wait()
        if i == 1:
            copy_dn(4).start()
            copy_dn(5, 0, 1).start()
        elif i >= 2:
            copy_dn(5, i - 1, 1).start()
        for c in chunks:
            up_chunk(c)
    n_step(0)
    e_start(1, e_finish(0))

    def finish_d(c):
        send_d(c).wait_recv()
        cs = pl.ds(c * CW, CW)
        y_ref[:, cs] = (xm[:, cs].astype(F32) + (dsend[c] + drecv[c])).astype(BF16)

    def finish_e():
        total = jnp.sqrt(e_finish(2))
        fe_ref[...] = total[:, :D].reshape(D)
        fh_ref[...] = total[:, D:].reshape(128)[:12]

    hooks = {
        1: lambda: n_step(1),
        2: lambda: e_start(2, e_finish(1)),
        3: lambda: n_step(2),
        4: finish_e,
    }

    for c in range(N_DN):
        acc = None
        n = DN_U if c < N_DN - 1 else 1
        for u in range(0, DN_U, n):
            copy_dn(c, u, n).wait()
            part = jnp.dot(act[:, pl.ds(u * UNIT, n * UNIT)],
                           wbuf[pl.ds((DN_B + DN_U * c + u) * UNIT, n * UNIT), :],
                           preferred_element_type=F32)
            acc = part if acc is None else acc + part
        dsend[c] = acc
        send_d(c).start()
        if c >= 2:
            finish_d(c - 2)
        if c in hooks:
            hooks[c]()
    finish_d(N_DN - 2)
    finish_d(N_DN - 1)
    n_step(3)

    for c in range(N_O):
        send_o(c).wait_send()
    for c in range(N_DN):
        send_d(c).wait_send()


def writer(y, fn, fh, fe, y_out, fn_out, fh_out, fe_out, sem):
    copies = [pltpu.make_async_copy(a, b, sem.at[i])
              for i, (a, b) in enumerate(((y, y_out), (fn, fn_out), (fh, fh_out), (fe, fe_out)))]
    for c in copies:
        c.start()
    for c in copies:
        c.wait()


def solution(mesh):
    dims = (4, 4, 4)

    def local_layer(hidden, positions, ln1_gain, ln1_bias, w_q, w_k, w_v, w_o, ln2_gain, ln2_bias, w_up, w_down):
        hbm = pl.BlockSpec(memory_space=pltpu.HBM)
        vmem = pl.BlockSpec(memory_space=pltpu.VMEM)
        y, fn, fh, fe = pl.pallas_call(
            functools.partial(body, dims),
            out_shape=(
                pltpu.VMEM((ROWS, D), BF16),
                pltpu.VMEM((FL,), F32),
                pltpu.VMEM((12,), F32),
                pltpu.VMEM((D,), F32),
            ),
            in_specs=[hbm] * 13,
            out_specs=(vmem, vmem, vmem, vmem),
            scratch_shapes=[
                pltpu.VMEM((NU * UNIT, CW), BF16),
                pltpu.VMEM((D,), BF16),
                pltpu.VMEM((D,), BF16),
                pltpu.VMEM((D,), BF16),
                pltpu.VMEM((D,), BF16),
                pltpu.VMEM((SEQ,), jnp.int32),
                pltpu.VMEM((1, HEAD_DIM), F32),
                pltpu.VMEM((ROWS, D), BF16),
                pltpu.VMEM((ROWS, D), BF16),
                pltpu.VMEM((ROWS, D), BF16),
                pltpu.VMEM((12 * ROWS, HEAD_DIM), BF16),
                pltpu.VMEM((4 * ROWS, HEAD_DIM), BF16),
                pltpu.VMEM((ROWS, KL), BF16),
                pltpu.VMEM((ROWS, QL), BF16),
                pltpu.VMEM((ROWS, FL), BF16),
                pltpu.VMEM((N_O, ROWS, CW), F32),
                pltpu.VMEM((N_O, ROWS, CW), F32),
                pltpu.VMEM((N_DN, ROWS, CW), F32),
                pltpu.VMEM((N_DN, ROWS, CW), F32),
                pltpu.VMEM((1, FL), F32),
                pltpu.VMEM((1, EH), F32),
                pltpu.VMEM((3, 4, 1, EH), F32),
                pltpu.VMEM((3, 3, 4, 1, PN), F32),
                pltpu.SemaphoreType.DMA((20,)),
                pltpu.SemaphoreType.DMA((N_DN + DN_U - 1,)),
                pltpu.SemaphoreType.DMA((7,)),
                pltpu.SemaphoreType.DMA((N_O + N_DN,)),
                pltpu.SemaphoreType.DMA((N_O + N_DN,)),
                pltpu.SemaphoreType.DMA((4, 3, 3)),
                pltpu.SemaphoreType.DMA((4, 3, 3)),
            ],
            compiler_params=pltpu.CompilerParams(
                collective_id=0, has_side_effects=True, vmem_limit_bytes=62 * 2**20),
            name="layer",
        )(hidden.reshape(ROWS, D), positions, jnp.asarray(inv_freq_row()), ln1_gain, ln1_bias, ln2_gain, ln2_bias,
          w_q, w_k, w_v, w_o, w_up, w_down)
        held = [pltpu.with_memory_space_constraint(v, pltpu.VMEM) for v in (y, fn, fh, fe)]
        y, fn, fh, fe = pl.pallas_call(
            writer,
            out_shape=tuple(jax.ShapeDtypeStruct(v.shape, v.dtype) for v in held),
            in_specs=[vmem] * 4,
            out_specs=(hbm,) * 4,
            scratch_shapes=[pltpu.SemaphoreType.DMA((4,))],
            name="writer",
        )(*held)
        return y.reshape(hidden.shape), fn, fh, fe

    weight_col = P(None, "tp")
    weight_row = P("tp", None)
    return jax.shard_map(
        local_layer,
        mesh=mesh,
        in_specs=(P("dp"), P(), P(), P(), weight_col, weight_col, weight_col, weight_row, P(), P(), weight_col, weight_row),
        out_specs=(P("dp"), P("tp"), P("tp"), P()),
        check_vma=False,
    )
```

```python
import functools

import jax
import jax.numpy as jnp
import numpy as np
from jax import lax
from jax.experimental import pallas as pl
from jax.experimental.pallas import tpu as pltpu
from jax.sharding import PartitionSpec as P

HEAD_DIM = 128
ROT_DIM = 64
ROPE_BASE = 10000.0
LN_EPS = 1e-5
MESH = pl.DeviceIdType.MESH
F32 = jnp.float32
BF16 = jnp.bfloat16

SEQ = 64
ROWS = 128
D = 3072
QL = 1536
KL = 512
FL = 4608
CW = 512
UNIT = 1536
NU = 32
N_O = D // CW
N_UP = FL // CW
NA = 6 * CW
N_DN = D // CW
DN_U = FL // UNIT
EH = D + 128

O_U = 10
UP_U = 16
DN_B = 2
TP_SEM = (0, 0, 0, 1, 1, 1, 2, 2, 3, 3, 4, 5)
UP_SEM = (0, 0, 0, 1, 1, 2, 3, 4)
DN_SEM = (7, 8, 9, 10, 11, 0, 1, 2)


def inv_freq_row():
    half = ROT_DIM // 2
    freq = ROPE_BASE ** (-2.0 * np.arange(half, dtype=np.float64) / ROT_DIM)
    return np.concatenate([freq, freq, np.zeros(HEAD_DIM - ROT_DIM)])[None, :].astype(np.float32)


def body(sizes, x_hbm, pos_hbm, freq_hbm, g1, b1, g2, b2, wq, wk, wv, wo, wup, wdn,
         y_ref, fn_ref, fh_ref, fe_ref,
         wbuf, ln0, ln1, ln2, ln3, posb, freqb, xb, hb, xm, qs, ks, vs, at, act, xsend, xrecv,
         nsc, esc, are, arn, arm,
         sem, tp_send, tp_recv, ar_send, ar_recv):
    dims = sizes
    tp = lax.axis_index("tp")
    dp = lax.axis_index("dp")
    sz, sy, sx = dims
    ix = lax.rem(dp, sx)
    iy = lax.rem(lax.div(dp, sx), sy)
    iz = lax.div(dp, sx * sy)
    partner = 1 - tp

    def peer(phase, k):
        step, flip = k // 2, k % 2
        if phase == 0:
            to_x, to_z = lax.rem(ix + step, sx), iz
            to_y = iy + 1 - 2 * lax.rem(iy, 2) if flip else iy
        else:
            to_x, to_z = ix, lax.rem(iz + step, sz)
            to_y = sy - 1 - iy if flip else iy
        return to_x + sx * (to_y + sy * to_z)

    place = (2 * ix + lax.rem(iy, 2), 2 * iz + lax.div(iy, 2))
    group_size = (2 * sx, 2 * sz)

    def slot(u, n):
        return wbuf.at[pl.ds(u * UNIT, n * UNIT), :]

    def cols(ref, c):
        return ref.at[:, pl.ds(c * CW, CW)]

    def arrive(u, n, s):
        pltpu.make_async_copy(slot(u, n), slot(u, n), sem.at[s]).wait()

    def copy_k():
        return pltpu.make_async_copy(wk, slot(6, 2), sem.at[7])

    def copy_v():
        return pltpu.make_async_copy(wv, slot(8, 2), sem.at[7])

    def copy_q(c):
        return pltpu.make_async_copy(cols(wq, c), slot(2 * c, 2), sem.at[8 + c // 2])

    def copy_o(c):
        return pltpu.make_async_copy(cols(wo, c), slot(O_U + c, 1), sem.at[10 + c // 3])

    def copy_up(c):
        return pltpu.make_async_copy(cols(wup, c), slot(UP_U + 2 * c, 2), sem.at[UP_SEM[c]])

    def copy_up_half(half):
        c = N_UP - 1
        return pltpu.make_async_copy(wup.at[pl.ds(half * UNIT, UNIT), pl.ds(c * CW, CW)],
                                     slot((UP_U + 2 * c) % NU + half, 1), sem.at[5 + half])

    def copy_dn(c, u=0, n=DN_U):
        return pltpu.make_async_copy(
            wdn.at[pl.ds(u * UNIT, n * UNIT), pl.ds(c * CW, CW)],
            slot(DN_B + DN_U * c + u, n), sem.at[DN_SEM[c + u]])

    def copy_x():
        return pltpu.make_async_copy(x_hbm, xb, sem.at[0])

    lnb = (ln0, ln1, ln2, ln3)
    small = [pltpu.make_async_copy(r, lnb[i], sem.at[1 + i]) for i, r in enumerate((g1, b1, g2, b2))]
    small.append(pltpu.make_async_copy(pos_hbm, posb, sem.at[5]))
    small.append(pltpu.make_async_copy(freq_hbm, freqb, sem.at[6]))

    barrier = pltpu.get_barrier_semaphore()
    greet = [{"tp": partner}]
    for phase in range(2):
        for k in range(1, group_size[phase]):
            greet.append({"dp": peer(phase, k)})
    first = [lambda: [copy_x().start()], lambda: [c.start() for c in small],
             lambda: [copy_k().start()], lambda: [copy_v().start()]]
    first += [lambda c=c: [copy_q(c).start()] for c in range(3)]
    first += [lambda c=c: [copy_o(c).start()] for c in range(N_O)]
    for i in range(max(len(first), len(greet))):
        if i < len(first):
            first[i]()
        if i < len(greet):
            pl.semaphore_signal(barrier, inc=1, device_id=greet[i], device_id_type=MESH)
    n_peers = len(greet)

    def layer_norm(src, dst, which):
        gain = 1.0 + lnb[2 * which][...].astype(F32).reshape(1, D)
        bias = lnb[2 * which + 1][...].astype(F32).reshape(1, D)
        total = None
        for b in range(ROWS // SEQ):
            acc = None
            for i in range(SEQ // 16):
                rows = pl.ds(b * SEQ + i * 16, 16)
                v = src[rows, :].astype(F32)
                mean = jnp.mean(v, axis=-1, keepdims=True)
                cen = v - mean
                var = jnp.mean(cen * cen, axis=-1, keepdims=True)
                h = (cen * lax.rsqrt(var + LN_EPS) * gain + bias).astype(BF16)
                dst[rows, :] = h
                hf = h.astype(F32)
                part = hf[:8] + hf[8:]
                acc = part if acc is None else acc + part
            mean_tok = jnp.sum(acc, axis=0, keepdims=True) * (1.0 / SEQ)
            sq = mean_tok * mean_tok
            total = sq if total is None else total + sq
        return total

    for c in small:
        c.wait()
    copy_x().wait()
    copy_up(0).start()
    copy_up(1).start()
    esc[:, pl.ds(0, D)] = layer_norm(xb, hb, 0)

    diag = (lax.broadcasted_iota(jnp.int32, (SEQ, SEQ), 0)
            == lax.broadcasted_iota(jnp.int32, (SEQ, SEQ), 1))
    pos_row = jnp.broadcast_to(posb[...].astype(F32).reshape(1, SEQ), (SEQ, SEQ))
    pos_col = jnp.sum(jnp.where(diag, pos_row, 0.0), axis=1, keepdims=True)
    angle = pos_col * freqb[...]
    cos, sin = jnp.cos(angle), jnp.sin(angle)
    hl = lax.broadcasted_iota(jnp.int32, (SEQ, HEAD_DIM), 1)
    keep = jnp.where(hl < ROT_DIM, cos, 1.0)
    from_right = jnp.where(hl < ROT_DIM // 2, -sin, 0.0)
    from_left = jnp.where((hl >= ROT_DIM // 2) & (hl < ROT_DIM), sin, 0.0)
    keep = jnp.concatenate([keep, keep], axis=0)
    from_right = jnp.concatenate([from_right, from_right], axis=0)
    from_left = jnp.concatenate([from_left, from_left], axis=0)

    def proj(u):
        return jnp.dot(hb[...], wbuf[pl.ds(u * UNIT, 2 * UNIT), :], preferred_element_type=F32)

    def rope(v):
        u = v.astype(BF16).astype(F32)
        r = pltpu.roll(u, HEAD_DIM - ROT_DIM // 2, 1)
        l = pltpu.roll(u, ROT_DIM // 2, 1)
        return (u * keep + r * from_right + l * from_left).astype(BF16)

    arrive(6, 4, 7)
    copy_up(2).start()
    copy_up(3).start()
    kk = proj(6)
    vv = proj(8)
    for g in range(4):
        ks[pl.ds(g * ROWS, ROWS), :] = rope(kk[:, g * HEAD_DIM:(g + 1) * HEAD_DIM])
    vs[...] = vv.astype(BF16)

    row = lax.broadcasted_iota(jnp.int32, (3 * ROWS, ROWS), 0) & (ROWS - 1)
    col = lax.broadcasted_iota(jnp.int32, (3 * ROWS, ROWS), 1)
    same = (row >= SEQ) == (col >= SEQ)
    allowed = same & (col <= row)
    blocked = jnp.where(same, F32(-1e30), F32(-jnp.inf))
    lane = lax.broadcasted_iota(jnp.int32, (1, ROWS), 1)

    def attention(g, head_sq):
        q = qs[pl.ds(g * 3 * ROWS, 3 * ROWS), :]
        k = ks[pl.ds(g * ROWS, ROWS), :]
        v = vs[:, g * HEAD_DIM:(g + 1) * HEAD_DIM]
        s = lax.dot_general(q, k, (((1,), (1,)), ((), ())), preferred_element_type=F32) * HEAD_DIM ** -0.5
        s = jnp.where(allowed, s, blocked)
        e = jnp.exp(s - jnp.max(s, axis=-1, keepdims=True))
        p = (e / jnp.sum(e, axis=-1, keepdims=True)).astype(BF16)
        o = jnp.dot(p, v, preferred_element_type=F32).astype(BF16)
        of = o.astype(F32)
        norm = jnp.sqrt(jnp.sum(of * of, axis=-1, keepdims=True))
        for j in range(3):
            i = 3 * g + j
            at[:, i * HEAD_DIM:(i + 1) * HEAD_DIM] = o[j * ROWS:(j + 1) * ROWS, :]
            m0 = jnp.sum(norm[j * ROWS:j * ROWS + SEQ], axis=0, keepdims=True) * (1.0 / SEQ)
            m1 = jnp.sum(norm[j * ROWS + SEQ:(j + 1) * ROWS], axis=0, keepdims=True) * (1.0 / SEQ)
            head_sq = head_sq + jnp.where(lane == i, m0 * m0 + m1 * m1, 0.0)
        return head_sq

    def query(c):
        qq = proj(2 * c)
        for j in range(4):
            qs[pl.ds((4 * c + j) * ROWS, ROWS), :] = rope(qq[:, j * HEAD_DIM:(j + 1) * HEAD_DIM])

    head_sq = jnp.zeros((1, ROWS), F32)
    arrive(0, 4, 8)
    copy_up(4).start()
    copy_up(5).start()
    query(0)
    query(1)
    head_sq = attention(0, head_sq)
    head_sq = attention(1, head_sq)
    arrive(4, 2, 9)
    copy_up(6).start()
    copy_up(7).start()
    copy_up_half(0).start()
    copy_up_half(1).start()
    query(2)
    head_sq = attention(2, head_sq)
    head_sq = attention(3, head_sq)
    esc[:, pl.ds(D, 128)] = head_sq

    def send(c):
        return pltpu.make_async_remote_copy(
            src_ref=xsend.at[c], dst_ref=xrecv.at[c], send_sem=tp_send, recv_sem=tp_recv.at[TP_SEM[c]],
            device_id={"tp": partner}, device_id_type=MESH)

    def receive(c, n):
        part = pl.ds(c, n)
        pltpu.make_async_remote_copy(
            src_ref=xsend.at[part], dst_ref=xrecv.at[part], send_sem=tp_send, recv_sem=tp_recv.at[TP_SEM[c]],
            device_id={"tp": partner}, device_id_type=MESH).wait_recv()

    pl.semaphore_wait(barrier, n_peers)

    for part in range(2):
        arrive(O_U + 3 * part, 3, 10 + part)
        if part == 0:
            copy_dn(0).start()
            copy_dn(1).start()
        else:
            copy_dn(2).start()
        for c in range(3 * part, 3 * part + 3):
            xsend[c] = jnp.dot(at[...], wbuf[pl.ds((O_U + c) * UNIT, UNIT), :], preferred_element_type=F32)
            send(c).start()
        if part == 1:
            copy_dn(3).start()
    for part in range(2):
        receive(3 * part, 3)
        for c in range(3 * part, 3 * part + 3):
            cs = pl.ds(c * CW, CW)
            xm[:, cs] = (xb[:, cs].astype(F32) + (xsend[c] + xrecv[c])).astype(BF16)

    esc[:, pl.ds(0, D)] = esc[:, pl.ds(0, D)] + layer_norm(xm, hb, 1)

    def ar_copy(buf, group, phase, src, k):
        return pltpu.make_async_remote_copy(
            src_ref=src, dst_ref=src, send_sem=ar_send.at[group], recv_sem=ar_recv.at[group, phase],
            device_id={"dp": peer(phase, k)}, device_id_type=MESH)

    def ar_start(buf, group, phase, value):
        buf[phase, place[phase]] = value
        for k in range(1, group_size[phase]):
            ar_copy(buf, group, phase, buf.at[phase, place[phase]], k).start()

    def ar_finish(buf, group, phase):
        ar_copy(buf, group, phase, buf.at[phase, pl.ds(0, group_size[phase] - 1)], 1).wait_recv()
        total = buf[phase, 0]
        for j in range(1, group_size[phase]):
            total = total + buf[phase, j]
        return total

    def ar_sent(buf, group):
        ar_copy(buf, group, 0, buf.at[:, pl.ds(0, group_size[0] - 1)], 1).wait_send()

    def e_finish():
        total = jnp.sqrt(ar_finish(are, 0, 1))
        fe_ref[...] = total[:, :D].reshape(D)
        fh_ref[...] = total[:, D:].reshape(128)[:12]

    def na_finish():
        fn_ref[pl.ds(0, NA)] = jnp.sqrt(ar_finish(arn, 1, 1)).reshape(NA)

    def nb_finish():
        fn_ref[pl.ds(NA, FL - NA)] = jnp.sqrt(ar_finish(arm, 2, 1)).reshape(FL - NA)

    ar_start(are, 0, 0, esc[...])

    def up_score(c, u):
        r = jnp.maximum(u, 0.0)
        a = r * r
        cs = pl.ds(c * CW, CW)
        act[:, cs] = a.astype(BF16)
        m0 = jnp.sum(a[:SEQ], axis=0, keepdims=True) * (1.0 / SEQ)
        m1 = jnp.sum(a[SEQ:], axis=0, keepdims=True) * (1.0 / SEQ)
        nsc[:, cs] = m0 * m0 + m1 * m1

    def up_dot(c, half, n):
        u0 = (UP_U + 2 * c) % NU + half
        return jnp.dot(hb[:, pl.ds(half * UNIT, n * UNIT)], wbuf[pl.ds(u0 * UNIT, n * UNIT), :],
                       preferred_element_type=F32)

    for i, chunks in enumerate(((0, 1, 2), (3, 4), (5,), (6,), (7,))):
        arrive(UP_U + 2 * chunks[0], 2 * len(chunks), UP_SEM[chunks[0]])
        if i == 1:
            copy_dn(4).start()
            copy_dn(5, 0, 1).start()
        elif i == 3:
            copy_dn(5, 1, 1).start()
            copy_dn(5, 2, 1).start()
        for c in chunks:
            up_score(c, up_dot(c, 0, 2))
        if i == 2:
            ar_start(arn, 1, 0, nsc[:, pl.ds(0, NA)])
    last = N_UP - 1
    copy_up_half(0).wait()
    u = up_dot(last, 0, 1)
    copy_up_half(1).wait()
    up_score(last, u + up_dot(last, 1, 1))
    ar_start(arm, 2, 0, nsc[:, pl.ds(NA, FL - NA)])

    def finish_d(first, n):
        receive(N_O + first, n)
        for c in range(first, first + n):
            cs = pl.ds(c * CW, CW)
            y_ref[:, cs] = (xm[:, cs].astype(F32) + (xsend[N_O + c] + xrecv[N_O + c])).astype(BF16)

    hooks = {
        0: lambda: ar_start(are, 0, 1, ar_finish(are, 0, 0)),
        1: lambda: ar_start(arn, 1, 1, ar_finish(arn, 1, 0)),
        2: lambda: ar_start(arm, 2, 1, ar_finish(arm, 2, 0)),
        5: lambda: (e_finish(), na_finish()),
    }

    for c in range(N_DN):
        acc = None
        n = DN_U if c < N_DN - 1 else 1
        for u in range(0, DN_U, n):
            copy_dn(c, u, n).wait()
            part = jnp.dot(act[:, pl.ds(u * UNIT, n * UNIT)],
                           wbuf[pl.ds((DN_B + DN_U * c + u) * UNIT, n * UNIT), :],
                           preferred_element_type=F32)
            acc = part if acc is None else acc + part
        xsend[N_O + c] = acc
        send(N_O + c).start()
        if c in (3, 5):
            finish_d(c - 3, 2)
        if c in hooks:
            hooks[c]()
    finish_d(N_DN - 2, 1)
    finish_d(N_DN - 1, 1)
    nb_finish()

    pltpu.make_async_remote_copy(
        src_ref=xsend, dst_ref=xrecv, send_sem=tp_send, recv_sem=tp_recv.at[0],
        device_id={"tp": partner}, device_id_type=MESH).wait_send()
    ar_sent(are, 0)
    ar_sent(arn, 1)
    ar_sent(arm, 2)


def writer(y, fn, fh, fe, y_out, fn_out, fh_out, fe_out, sem):
    copies = [pltpu.make_async_copy(a, b, sem.at[i])
              for i, (a, b) in enumerate(((y, y_out), (fn, fn_out), (fh, fh_out), (fe, fe_out)))]
    for c in copies:
        c.start()
    for c in copies:
        c.wait()


def solution(mesh):
    dims = (4, 4, 4)

    def local_layer(hidden, positions, ln1_gain, ln1_bias, w_q, w_k, w_v, w_o, ln2_gain, ln2_bias, w_up, w_down):
        hbm = pl.BlockSpec(memory_space=pltpu.HBM)
        vmem = pl.BlockSpec(memory_space=pltpu.VMEM)
        y, fn, fh, fe = pl.pallas_call(
            functools.partial(body, dims),
            out_shape=(
                pltpu.VMEM((ROWS, D), BF16),
                pltpu.VMEM((FL,), F32),
                pltpu.VMEM((12,), F32),
                pltpu.VMEM((D,), F32),
            ),
            in_specs=[hbm] * 13,
            out_specs=(vmem, vmem, vmem, vmem),
            scratch_shapes=[
                pltpu.VMEM((NU * UNIT, CW), BF16),
                pltpu.VMEM((D,), BF16),
                pltpu.VMEM((D,), BF16),
                pltpu.VMEM((D,), BF16),
                pltpu.VMEM((D,), BF16),
                pltpu.VMEM((SEQ,), jnp.int32),
                pltpu.VMEM((1, HEAD_DIM), F32),
                pltpu.VMEM((ROWS, D), BF16),
                pltpu.VMEM((ROWS, D), BF16),
                pltpu.VMEM((ROWS, D), BF16),
                pltpu.VMEM((12 * ROWS, HEAD_DIM), BF16),
                pltpu.VMEM((4 * ROWS, HEAD_DIM), BF16),
                pltpu.VMEM((ROWS, KL), BF16),
                pltpu.VMEM((ROWS, QL), BF16),
                pltpu.VMEM((ROWS, FL), BF16),
                pltpu.VMEM((N_O + N_DN, ROWS, CW), F32),
                pltpu.VMEM((N_O + N_DN, ROWS, CW), F32),
                pltpu.VMEM((1, FL), F32),
                pltpu.VMEM((1, EH), F32),
                pltpu.VMEM((2, 8, 1, EH), F32),
                pltpu.VMEM((2, 8, 1, NA), F32),
                pltpu.VMEM((2, 8, 1, FL - NA), F32),
                pltpu.SemaphoreType.DMA((12,)),
                pltpu.SemaphoreType.DMA,
                pltpu.SemaphoreType.DMA((6,)),
                pltpu.SemaphoreType.DMA((3,)),
                pltpu.SemaphoreType.DMA((3, 2)),
            ],
            compiler_params=pltpu.CompilerParams(
                collective_id=0, has_side_effects=True, vmem_limit_bytes=62 * 2**20),
            name="layer",
        )(hidden.reshape(ROWS, D), positions, jnp.asarray(inv_freq_row()), ln1_gain, ln1_bias, ln2_gain, ln2_bias,
          w_q, w_k, w_v, w_o, w_up, w_down)
        held = [pltpu.with_memory_space_constraint(v, pltpu.VMEM) for v in (y, fn, fh, fe)]
        y, fn, fh, fe = pl.pallas_call(
            writer,
            out_shape=tuple(jax.ShapeDtypeStruct(v.shape, v.dtype) for v in held),
            in_specs=[vmem] * 4,
            out_specs=(hbm,) * 4,
            scratch_shapes=[pltpu.SemaphoreType.DMA((4,))],
            name="writer",
        )(*held)
        return y.reshape(hidden.shape), fn, fh, fe

    weight_col = P(None, "tp")
    weight_row = P("tp", None)
    return jax.shard_map(
        local_layer,
        mesh=mesh,
        in_specs=(P("dp"), P(), P(), P(), weight_col, weight_col, weight_col, weight_row, P(), P(), weight_col, weight_row),
        out_specs=(P("dp"), P("tp"), P("tp"), P()),
        check_vma=False,
    )
```

```python
import functools

import jax
import jax.numpy as jnp
import numpy as np
from jax import lax
from jax.experimental import pallas as pl
from jax.experimental.pallas import tpu as pltpu
from jax.sharding import PartitionSpec as P

HEAD_DIM = 128
ROT_DIM = 64
ROPE_BASE = 10000.0
LN_EPS = 1e-5
MESH = pl.DeviceIdType.MESH
F32 = jnp.float32
BF16 = jnp.bfloat16

SEQ = 64
ROWS = 128
D = 3072
QL = 1536
KL = 512
FL = 4608
CW = 512
UNIT = 1536
NU = 32
N_O = D // CW
N_UP = FL // CW
NA = 6 * CW
N_DN = D // CW
DN_U = FL // UNIT
EH = D + 128

O_U = 10
UP_U = 16
DN_B = 2
TP_SEM = (0, 0, 0, 1, 1, 1, 2, 2, 3, 3, 4, 5)
UP_SEM = (0, 0, 0, 1, 1, 2, 3, 4)
UP_LAST = ((0, 1536, 5), (1536, 768, 6), (2304, 768, 12))
DN_SEM = (7, 8, 9, 10, 11, 0, 1, 2)


def inv_freq_row():
    half = ROT_DIM // 2
    freq = ROPE_BASE ** (-2.0 * np.arange(half, dtype=np.float64) / ROT_DIM)
    return np.concatenate([freq, freq, np.zeros(HEAD_DIM - ROT_DIM)])[None, :].astype(np.float32)


def body(sizes, x_hbm, pos_hbm, freq_hbm, g1, b1, g2, b2, wq, wk, wv, wo, wup, wdn,
         y_ref, fn_ref, fh_ref, fe_ref,
         wbuf, ln0, ln1, ln2, ln3, posb, freqb, xb, hb, xm, qs, ks, vs, at, act, xsend, xrecv,
         nsc, esc, are, arn, arm, ars, stage,
         sem, tp_send, tp_recv, ar_send, ar_recv):
    dims = sizes
    tp = lax.axis_index("tp")
    dp = lax.axis_index("dp")
    sz, sy, sx = dims
    ix = lax.rem(dp, sx)
    iy = lax.rem(lax.div(dp, sx), sy)
    iz = lax.div(dp, sx * sy)
    partner = 1 - tp

    def peer(phase, k):
        step, flip = k // 2, k % 2
        if phase == 0:
            to_x, to_z = lax.rem(ix + step, sx), iz
            to_y = sy - 1 - iy if flip else iy
        else:
            to_x, to_z = ix, lax.rem(iz + step, sz)
            to_y = iy + 1 - 2 * lax.rem(iy, 2) if flip else iy
        return to_x + sx * (to_y + sy * to_z)

    place = (2 * ix + lax.div(iy, 2), 2 * iz + lax.rem(lax.div(iy + 1, 2), 2))
    group_size = (2 * sx, 2 * sz)

    def slot(u, n):
        return wbuf.at[pl.ds(u * UNIT, n * UNIT), :]

    def cols(ref, c):
        return ref.at[:, pl.ds(c * CW, CW)]

    def arrive(u, n, s):
        pltpu.make_async_copy(slot(u, n), slot(u, n), sem.at[s]).wait()

    def copy_k():
        return pltpu.make_async_copy(wk, slot(6, 2), sem.at[7])

    def copy_v():
        return pltpu.make_async_copy(wv, slot(8, 2), sem.at[7])

    def copy_q(c):
        return pltpu.make_async_copy(cols(wq, c), slot(2 * c, 2), sem.at[8 + c // 2])

    def copy_o(c):
        return pltpu.make_async_copy(cols(wo, c), slot(O_U + c, 1), sem.at[10 + c // 3])

    def copy_up(c):
        return pltpu.make_async_copy(cols(wup, c), slot(UP_U + 2 * c, 2), sem.at[UP_SEM[c]])

    def copy_up_last(r0, n, i):
        return pltpu.make_async_copy(wup.at[pl.ds(r0, n), pl.ds((N_UP - 1) * CW, CW)],
                                     wbuf.at[pl.ds(r0, n), :], sem.at[i])

    def copy_dn(c, u=0, n=DN_U):
        return pltpu.make_async_copy(
            wdn.at[pl.ds(u * UNIT, n * UNIT), pl.ds(c * CW, CW)],
            slot(DN_B + DN_U * c + u, n), sem.at[DN_SEM[c + u]])

    def copy_x():
        return pltpu.make_async_copy(x_hbm, xb, sem.at[0])

    lnb = (ln0, ln1, ln2, ln3)
    small = [pltpu.make_async_copy(r, lnb[i], sem.at[1 + i]) for i, r in enumerate((g1, b1, g2, b2))]
    small.append(pltpu.make_async_copy(pos_hbm, posb, sem.at[5]))
    small.append(pltpu.make_async_copy(freq_hbm, freqb, sem.at[6]))

    barrier = pltpu.get_barrier_semaphore()
    greet = [{"tp": partner}]
    for phase in range(2):
        for k in range(1, group_size[phase]):
            greet.append({"dp": peer(phase, k)})
            greet.append({"dp": peer(phase, k), "tp": partner})
    first = [lambda: [copy_x().start()], lambda: [c.start() for c in small],
             lambda: [copy_k().start()], lambda: [copy_v().start()]]
    first += [lambda c=c: [copy_q(c).start()] for c in range(3)]
    first += [lambda c=c: [copy_o(c).start()] for c in range(N_O)]
    for i in range(max(len(first), len(greet))):
        if i < len(first):
            first[i]()
        if i < len(greet):
            pl.semaphore_signal(barrier, inc=1, device_id=greet[i], device_id_type=MESH)
    n_peers = len(greet)

    def layer_norm(src, dst, which):
        gain = 1.0 + lnb[2 * which][...].astype(F32).reshape(1, D)
        bias = lnb[2 * which + 1][...].astype(F32).reshape(1, D)
        total = None
        for b in range(ROWS // SEQ):
            acc = None
            for i in range(SEQ // 16):
                rows = pl.ds(b * SEQ + i * 16, 16)
                v = src[rows, :].astype(F32)
                mean = jnp.mean(v, axis=-1, keepdims=True)
                cen = v - mean
                var = jnp.mean(cen * cen, axis=-1, keepdims=True)
                h = (cen * lax.rsqrt(var + LN_EPS) * gain + bias).astype(BF16)
                dst[rows, :] = h
                hf = h.astype(F32)
                part = hf[:8] + hf[8:]
                acc = part if acc is None else acc + part
            mean_tok = jnp.sum(acc, axis=0, keepdims=True) * (1.0 / SEQ)
            sq = mean_tok * mean_tok
            total = sq if total is None else total + sq
        return total

    for c in small:
        c.wait()
    copy_x().wait()
    copy_up(0).start()
    copy_up(1).start()
    esc[:, pl.ds(0, D)] = layer_norm(xb, hb, 0)

    diag = (lax.broadcasted_iota(jnp.int32, (SEQ, SEQ), 0)
            == lax.broadcasted_iota(jnp.int32, (SEQ, SEQ), 1))
    pos_row = jnp.broadcast_to(posb[...].astype(F32).reshape(1, SEQ), (SEQ, SEQ))
    pos_col = jnp.sum(jnp.where(diag, pos_row, 0.0), axis=1, keepdims=True)
    angle = pos_col * freqb[...]
    cos, sin = jnp.cos(angle), jnp.sin(angle)
    hl = lax.broadcasted_iota(jnp.int32, (SEQ, HEAD_DIM), 1)
    keep = jnp.where(hl < ROT_DIM, cos, 1.0)
    from_right = jnp.where(hl < ROT_DIM // 2, -sin, 0.0)
    from_left = jnp.where((hl >= ROT_DIM // 2) & (hl < ROT_DIM), sin, 0.0)
    keep = jnp.concatenate([keep, keep], axis=0)
    from_right = jnp.concatenate([from_right, from_right], axis=0)
    from_left = jnp.concatenate([from_left, from_left], axis=0)

    def proj(u):
        return jnp.dot(hb[...], wbuf[pl.ds(u * UNIT, 2 * UNIT), :], preferred_element_type=F32)

    def rope(v):
        u = v.astype(BF16).astype(F32)
        r = pltpu.roll(u, HEAD_DIM - ROT_DIM // 2, 1)
        l = pltpu.roll(u, ROT_DIM // 2, 1)
        return (u * keep + r * from_right + l * from_left).astype(BF16)

    arrive(6, 4, 7)
    copy_up(2).start()
    copy_up(3).start()
    kk = proj(6)
    vv = proj(8)
    for g in range(4):
        ks[pl.ds(g * ROWS, ROWS), :] = rope(kk[:, g * HEAD_DIM:(g + 1) * HEAD_DIM])
    vs[...] = vv.astype(BF16)

    row = lax.broadcasted_iota(jnp.int32, (3 * ROWS, ROWS), 0) & (ROWS - 1)
    col = lax.broadcasted_iota(jnp.int32, (3 * ROWS, ROWS), 1)
    same = (row >= SEQ) == (col >= SEQ)
    allowed = same & (col <= row)
    blocked = jnp.where(same, F32(-1e30), F32(-jnp.inf))
    lane = lax.broadcasted_iota(jnp.int32, (1, ROWS), 1)

    def attention(g, head_sq):
        q = qs[pl.ds(g * 3 * ROWS, 3 * ROWS), :]
        k = ks[pl.ds(g * ROWS, ROWS), :]
        v = vs[:, g * HEAD_DIM:(g + 1) * HEAD_DIM]
        s = lax.dot_general(q, k, (((1,), (1,)), ((), ())), preferred_element_type=F32) * HEAD_DIM ** -0.5
        s = jnp.where(allowed, s, blocked)
        e = jnp.exp(s - jnp.max(s, axis=-1, keepdims=True))
        p = (e / jnp.sum(e, axis=-1, keepdims=True)).astype(BF16)
        o = jnp.dot(p, v, preferred_element_type=F32).astype(BF16)
        of = o.astype(F32)
        norm = jnp.sqrt(jnp.sum(of * of, axis=-1, keepdims=True))
        for j in range(3):
            i = 3 * g + j
            at[:, i * HEAD_DIM:(i + 1) * HEAD_DIM] = o[j * ROWS:(j + 1) * ROWS, :]
            m0 = jnp.sum(norm[j * ROWS:j * ROWS + SEQ], axis=0, keepdims=True) * (1.0 / SEQ)
            m1 = jnp.sum(norm[j * ROWS + SEQ:(j + 1) * ROWS], axis=0, keepdims=True) * (1.0 / SEQ)
            head_sq = head_sq + jnp.where(lane == i, m0 * m0 + m1 * m1, 0.0)
        return head_sq

    def query(c):
        qq = proj(2 * c)
        for j in range(4):
            qs[pl.ds((4 * c + j) * ROWS, ROWS), :] = rope(qq[:, j * HEAD_DIM:(j + 1) * HEAD_DIM])

    head_sq = jnp.zeros((1, ROWS), F32)
    arrive(0, 4, 8)
    copy_up(4).start()
    copy_up(5).start()
    query(0)
    query(1)
    head_sq = attention(0, head_sq)
    head_sq = attention(1, head_sq)
    arrive(4, 2, 9)
    copy_up(6).start()
    copy_up(7).start()
    for r0, n, i in UP_LAST:
        copy_up_last(r0, n, i).start()
    query(2)
    head_sq = attention(2, head_sq)
    head_sq = attention(3, head_sq)
    esc[:, pl.ds(D, 128)] = head_sq

    def send(c):
        return pltpu.make_async_remote_copy(
            src_ref=xsend.at[c], dst_ref=xrecv.at[c], send_sem=tp_send, recv_sem=tp_recv.at[TP_SEM[c]],
            device_id={"tp": partner}, device_id_type=MESH)

    def receive(c, n):
        part = pl.ds(c, n)
        pltpu.make_async_remote_copy(
            src_ref=xsend.at[part], dst_ref=xrecv.at[part], send_sem=tp_send, recv_sem=tp_recv.at[TP_SEM[c]],
            device_id={"tp": partner}, device_id_type=MESH).wait_recv()

    pl.semaphore_wait(barrier, n_peers)

    for part in range(2):
        arrive(O_U + 3 * part, 3, 10 + part)
        if part == 0:
            copy_dn(0).start()
            copy_dn(1).start()
        else:
            copy_dn(2).start()
        for c in range(3 * part, 3 * part + 3):
            xsend[c] = jnp.dot(at[...], wbuf[pl.ds((O_U + c) * UNIT, UNIT), :], preferred_element_type=F32)
            send(c).start()
        if part == 1:
            copy_dn(3).start()
    for part in range(2):
        receive(3 * part, 3)
        for c in range(3 * part, 3 * part + 3):
            cs = pl.ds(c * CW, CW)
            xm[:, cs] = (xb[:, cs].astype(F32) + (xsend[c] + xrecv[c])).astype(BF16)

    esc[:, pl.ds(0, D)] = esc[:, pl.ds(0, D)] + layer_norm(xm, hb, 1)

    def ar_copy(buf, group, phase, src, k):
        return pltpu.make_async_remote_copy(
            src_ref=src, dst_ref=src, send_sem=ar_send.at[group], recv_sem=ar_recv.at[group, phase],
            device_id={"dp": peer(phase, k)}, device_id_type=MESH)

    def ar_start(buf, group, phase, value):
        buf[phase, place[phase]] = value
        for k in range(1, group_size[phase]):
            ar_copy(buf, group, phase, buf.at[phase, place[phase]], k).start()

    def ar_finish(buf, group, phase):
        ar_copy(buf, group, phase, buf.at[phase, pl.ds(0, group_size[phase] - 1)], 1).wait_recv()
        total = buf[phase, 0]
        for j in range(1, group_size[phase]):
            total = total + buf[phase, j]
        return total

    def ar_sent(buf, group):
        ar_copy(buf, group, 0, buf.at[:, pl.ds(0, group_size[0] - 1)], 1).wait_send()

    def e_finish():
        total = jnp.sqrt(ar_finish(are, 0, 1))
        fe_ref[...] = total[:, :D].reshape(D)
        fh_ref[...] = total[:, D:].reshape(128)[:12]

    def na_finish():
        fn_ref[pl.ds(0, NA)] = jnp.sqrt(ar_finish(arn, 1, 1)).reshape(NA)

    NB = FL - NA

    def cross_copy(phase, src, dst, k):
        return pltpu.make_async_remote_copy(
            src_ref=src, dst_ref=dst, send_sem=ar_send.at[3], recv_sem=ar_recv.at[3, phase],
            device_id={"dp": peer(phase, k) if k else dp, "tp": partner}, device_id_type=MESH)

    def cross_start(phase, src):
        for k in range(group_size[phase]):
            cross_copy(phase, src, ars.at[phase, place[phase]], k).start()

    def cross_finish(phase):
        cross_copy(phase, ars.at[phase], ars.at[phase], 0).wait_recv()
        total = ars[phase, 0]
        for j in range(1, group_size[phase]):
            total = total + ars[phase, j]
        return total

    def nb_start():
        @pl.when(tp == 0)
        def _():
            cross_start(0, nsc.at[:, pl.ds(NA, NB)])

        @pl.when(tp == 1)
        def _():
            ar_start(arm, 2, 0, nsc[:, pl.ds(NA, NB)])

    def nb_middle():
        @pl.when(tp == 1)
        def _():
            stage[...] = cross_finish(0)
            cross_start(1, stage)
            ar_start(arm, 2, 1, ar_finish(arm, 2, 0))

    def nb_finish():
        @pl.when(tp == 0)
        def _():
            fn_ref[pl.ds(NA, NB)] = jnp.sqrt(cross_finish(1)).reshape(NB)

        @pl.when(tp == 1)
        def _():
            fn_ref[pl.ds(NA, NB)] = jnp.sqrt(ar_finish(arm, 2, 1)).reshape(NB)
            ar_sent(arm, 2)
        cross_copy(0, ars.at[0], ars.at[0], 0).wait_send()

    ar_start(are, 0, 0, esc[...])

    def up_score(c, u):
        r = jnp.maximum(u, 0.0)
        a = r * r
        cs = pl.ds(c * CW, CW)
        act[:, cs] = a.astype(BF16)
        m0 = jnp.sum(a[:SEQ], axis=0, keepdims=True) * (1.0 / SEQ)
        m1 = jnp.sum(a[SEQ:], axis=0, keepdims=True) * (1.0 / SEQ)
        nsc[:, cs] = m0 * m0 + m1 * m1

    def up_dot(c):
        return jnp.dot(hb[...], wbuf[pl.ds((UP_U + 2 * c) * UNIT, 2 * UNIT), :], preferred_element_type=F32)

    for i, chunks in enumerate(((0, 1, 2), (3, 4), (5,), (6,), (7,))):
        arrive(UP_U + 2 * chunks[0], 2 * len(chunks), UP_SEM[chunks[0]])
        if i == 1:
            copy_dn(4).start()
            copy_dn(5, 0, 1).start()
        elif i == 3:
            copy_dn(5, 1, 1).start()
            copy_dn(5, 2, 1).start()
        for c in chunks:
            up_score(c, up_dot(c))
        if i == 2:
            ar_start(arn, 1, 0, nsc[:, pl.ds(0, NA)])
    u = None
    for r0, n, i in UP_LAST:
        copy_up_last(r0, n, i).wait()
        part = jnp.dot(hb[:, pl.ds(r0, n)], wbuf[pl.ds(r0, n), :], preferred_element_type=F32)
        u = part if u is None else u + part
    up_score(N_UP - 1, u)
    nb_start()

    def finish_d(first, n):
        receive(N_O + first, n)
        for c in range(first, first + n):
            cs = pl.ds(c * CW, CW)
            y_ref[:, cs] = (xm[:, cs].astype(F32) + (xsend[N_O + c] + xrecv[N_O + c])).astype(BF16)

    hooks = {
        0: lambda: ar_start(are, 0, 1, ar_finish(are, 0, 0)),
        1: lambda: ar_start(arn, 1, 1, ar_finish(arn, 1, 0)),
        2: nb_middle,
        5: lambda: (e_finish(), na_finish()),
    }

    for c in range(N_DN):
        acc = None
        n = DN_U if c < N_DN - 1 else 1
        for u in range(0, DN_U, n):
            copy_dn(c, u, n).wait()
            part = jnp.dot(act[:, pl.ds(u * UNIT, n * UNIT)],
                           wbuf[pl.ds((DN_B + DN_U * c + u) * UNIT, n * UNIT), :],
                           preferred_element_type=F32)
            acc = part if acc is None else acc + part
        xsend[N_O + c] = acc
        send(N_O + c).start()
        if c in (3, 5):
            finish_d(c - 3, 2)
        if c in hooks:
            hooks[c]()
    finish_d(N_DN - 2, 1)
    finish_d(N_DN - 1, 1)
    nb_finish()

    pltpu.make_async_remote_copy(
        src_ref=xsend, dst_ref=xrecv, send_sem=tp_send, recv_sem=tp_recv.at[0],
        device_id={"tp": partner}, device_id_type=MESH).wait_send()
    ar_sent(are, 0)
    ar_sent(arn, 1)


def writer(y, fn, fh, fe, y_out, fn_out, fh_out, fe_out, sem):
    copies = [pltpu.make_async_copy(a, b, sem.at[i])
              for i, (a, b) in enumerate(((y, y_out), (fn, fn_out), (fh, fh_out), (fe, fe_out)))]
    for c in copies:
        c.start()
    for c in copies:
        c.wait()


def solution(mesh):
    dims = (4, 4, 4)

    def local_layer(hidden, positions, ln1_gain, ln1_bias, w_q, w_k, w_v, w_o, ln2_gain, ln2_bias, w_up, w_down):
        hbm = pl.BlockSpec(memory_space=pltpu.HBM)
        vmem = pl.BlockSpec(memory_space=pltpu.VMEM)
        y, fn, fh, fe = pl.pallas_call(
            functools.partial(body, dims),
            out_shape=(
                pltpu.VMEM((ROWS, D), BF16),
                pltpu.VMEM((FL,), F32),
                pltpu.VMEM((12,), F32),
                pltpu.VMEM((D,), F32),
            ),
            in_specs=[hbm] * 13,
            out_specs=(vmem, vmem, vmem, vmem),
            scratch_shapes=[
                pltpu.VMEM((NU * UNIT, CW), BF16),
                pltpu.VMEM((D,), BF16),
                pltpu.VMEM((D,), BF16),
                pltpu.VMEM((D,), BF16),
                pltpu.VMEM((D,), BF16),
                pltpu.VMEM((SEQ,), jnp.int32),
                pltpu.VMEM((1, HEAD_DIM), F32),
                pltpu.VMEM((ROWS, D), BF16),
                pltpu.VMEM((ROWS, D), BF16),
                pltpu.VMEM((ROWS, D), BF16),
                pltpu.VMEM((12 * ROWS, HEAD_DIM), BF16),
                pltpu.VMEM((4 * ROWS, HEAD_DIM), BF16),
                pltpu.VMEM((ROWS, KL), BF16),
                pltpu.VMEM((ROWS, QL), BF16),
                pltpu.VMEM((ROWS, FL), BF16),
                pltpu.VMEM((N_O + N_DN, ROWS, CW), F32),
                pltpu.VMEM((N_O + N_DN, ROWS, CW), F32),
                pltpu.VMEM((1, FL), F32),
                pltpu.VMEM((1, EH), F32),
                pltpu.VMEM((2, 8, 1, EH), F32),
                pltpu.VMEM((2, 8, 1, NA), F32),
                pltpu.VMEM((2, 8, 1, FL - NA), F32),
                pltpu.VMEM((2, 8, 1, FL - NA), F32),
                pltpu.VMEM((1, FL - NA), F32),
                pltpu.SemaphoreType.DMA((13,)),
                pltpu.SemaphoreType.DMA,
                pltpu.SemaphoreType.DMA((6,)),
                pltpu.SemaphoreType.DMA((4,)),
                pltpu.SemaphoreType.DMA((4, 2)),
            ],
            compiler_params=pltpu.CompilerParams(
                collective_id=0, has_side_effects=True, vmem_limit_bytes=62 * 2**20),
            name="layer",
        )(hidden.reshape(ROWS, D), positions, jnp.asarray(inv_freq_row()), ln1_gain, ln1_bias, ln2_gain, ln2_bias,
          w_q, w_k, w_v, w_o, w_up, w_down)
        held = [pltpu.with_memory_space_constraint(v, pltpu.VMEM) for v in (y, fn, fh, fe)]
        y, fn, fh, fe = pl.pallas_call(
            writer,
            out_shape=tuple(jax.ShapeDtypeStruct(v.shape, v.dtype) for v in held),
            in_specs=[vmem] * 4,
            out_specs=(hbm,) * 4,
            scratch_shapes=[pltpu.SemaphoreType.DMA((4,))],
            name="writer",
        )(*held)
        return y.reshape(hidden.shape), fn, fh, fe

    weight_col = P(None, "tp")
    weight_row = P("tp", None)
    return jax.shard_map(
        local_layer,
        mesh=mesh,
        in_specs=(P("dp"), P(), P(), P(), weight_col, weight_col, weight_col, weight_row, P(), P(), weight_col, weight_row),
        out_specs=(P("dp"), P("tp"), P("tp"), P()),
        check_vma=False,
    )
```

```python
import functools

import jax
import jax.numpy as jnp
import numpy as np
from jax import lax
from jax.experimental import pallas as pl
from jax.experimental.pallas import tpu as pltpu
from jax.sharding import PartitionSpec as P

HEAD_DIM = 128
ROT_DIM = 64
ROPE_BASE = 10000.0
LN_EPS = 1e-5
MESH = pl.DeviceIdType.MESH
F32 = jnp.float32
BF16 = jnp.bfloat16

SEQ = 64
ROWS = 128
D = 3072
QL = 1536
KL = 512
FL = 4608
CW = 512
UNIT = 1536
NU = 32
N_O = D // CW
N_UP = FL // CW
NA = 6 * CW
N_DN = D // CW
DN_U = FL // UNIT
EH = D + 128

O_U = 10
UP_U = 16
DN_B = 2
TP_SEM = (0, 0, 0, 1, 1, 1, 2, 2, 3, 3, 4, 5)
UP_SEM = (0, 0, 0, 1, 1, 2, 3, 4)
UP_LAST = ((0, 2304, 5), (2304, 768, 6))
DN_SEM = (7, 8, 9, 10, 11, 0, 1, 2)


def inv_freq_row():
    half = ROT_DIM // 2
    freq = ROPE_BASE ** (-2.0 * np.arange(half, dtype=np.float64) / ROT_DIM)
    return np.concatenate([freq, freq, np.zeros(HEAD_DIM - ROT_DIM)])[None, :].astype(np.float32)


def body(sizes, x_hbm, pos_hbm, freq_hbm, g1, b1, g2, b2, wq, wk, wv, wo, wup, wdn,
         y_ref, fn_ref, fh_ref, fe_ref,
         wbuf, ln0, ln1, ln2, ln3, posb, freqb, xb, hb, xm, qs, ks, vs, at, act, xsend, xrecv,
         nsc, esc, are, arn, arm, ars, stage,
         sem, tp_send, tp_recv, ar_send, ar_recv):
    dims = sizes
    tp = lax.axis_index("tp")
    dp = lax.axis_index("dp")
    sz, sy, sx = dims
    ix = lax.rem(dp, sx)
    iy = lax.rem(lax.div(dp, sx), sy)
    iz = lax.div(dp, sx * sy)
    partner = 1 - tp

    def peer(phase, k):
        step, flip = k // 2, k % 2
        if phase == 0:
            to_x, to_z = lax.rem(ix + step, sx), iz
            to_y = sy - 1 - iy if flip else iy
        else:
            to_x, to_z = ix, lax.rem(iz + step, sz)
            to_y = iy + 1 - 2 * lax.rem(iy, 2) if flip else iy
        return to_x + sx * (to_y + sy * to_z)

    place = (2 * ix + lax.div(iy, 2), 2 * iz + lax.rem(lax.div(iy + 1, 2), 2))
    group_size = (2 * sx, 2 * sz)

    def slot(u, n):
        return wbuf.at[pl.ds(u * UNIT, n * UNIT), :]

    def cols(ref, c):
        return ref.at[:, pl.ds(c * CW, CW)]

    def arrive(u, n, s):
        pltpu.make_async_copy(slot(u, n), slot(u, n), sem.at[s]).wait()

    def copy_k():
        return pltpu.make_async_copy(wk, slot(6, 2), sem.at[7])

    def copy_v():
        return pltpu.make_async_copy(wv, slot(8, 2), sem.at[7])

    def copy_q(c):
        return pltpu.make_async_copy(cols(wq, c), slot(2 * c, 2), sem.at[8 + c // 2])

    def copy_o(c):
        return pltpu.make_async_copy(cols(wo, c), slot(O_U + c, 1), sem.at[10 + c // 3])

    def copy_up(c):
        return pltpu.make_async_copy(cols(wup, c), slot(UP_U + 2 * c, 2), sem.at[UP_SEM[c]])

    def copy_up_last(r0, n, i):
        return pltpu.make_async_copy(wup.at[pl.ds(r0, n), pl.ds((N_UP - 1) * CW, CW)],
                                     wbuf.at[pl.ds(r0, n), :], sem.at[i])

    def copy_dn(c, u=0, n=DN_U):
        return pltpu.make_async_copy(
            wdn.at[pl.ds(u * UNIT, n * UNIT), pl.ds(c * CW, CW)],
            slot(DN_B + DN_U * c + u, n), sem.at[DN_SEM[c + u]])

    def copy_x():
        return pltpu.make_async_copy(x_hbm, xb, sem.at[0])

    lnb = (ln0, ln1, ln2, ln3)
    small = [pltpu.make_async_copy(r, lnb[i], sem.at[1 + i]) for i, r in enumerate((g1, b1, g2, b2))]
    small.append(pltpu.make_async_copy(pos_hbm, posb, sem.at[5]))
    small.append(pltpu.make_async_copy(freq_hbm, freqb, sem.at[6]))

    barrier = pltpu.get_barrier_semaphore()
    greet = [{"tp": partner}]
    for phase in range(2):
        for k in range(1, group_size[phase]):
            greet.append({"dp": peer(phase, k)})
            greet.append({"dp": peer(phase, k), "tp": partner})
    first = [lambda: [copy_x().start()], lambda: [c.start() for c in small],
             lambda: [copy_k().start()], lambda: [copy_v().start()]]
    first += [lambda c=c: [copy_q(c).start()] for c in range(3)]
    first += [lambda c=c: [copy_o(c).start()] for c in range(N_O)]
    for i in range(max(len(first), len(greet))):
        if i < len(first):
            first[i]()
        if i < len(greet):
            pl.semaphore_signal(barrier, inc=1, device_id=greet[i], device_id_type=MESH)
    n_peers = len(greet)

    def layer_norm(src, dst, which):
        gain = 1.0 + lnb[2 * which][...].astype(F32).reshape(1, D)
        bias = lnb[2 * which + 1][...].astype(F32).reshape(1, D)
        total = None
        for b in range(ROWS // SEQ):
            acc = None
            for i in range(SEQ // 16):
                rows = pl.ds(b * SEQ + i * 16, 16)
                v = src[rows, :].astype(F32)
                mean = jnp.mean(v, axis=-1, keepdims=True)
                cen = v - mean
                var = jnp.mean(cen * cen, axis=-1, keepdims=True)
                h = (cen * lax.rsqrt(var + LN_EPS) * gain + bias).astype(BF16)
                dst[rows, :] = h
                hf = h.astype(F32)
                part = hf[:8] + hf[8:]
                acc = part if acc is None else acc + part
            mean_tok = jnp.sum(acc, axis=0, keepdims=True) * (1.0 / SEQ)
            sq = mean_tok * mean_tok
            total = sq if total is None else total + sq
        return total

    for c in small:
        c.wait()
    copy_x().wait()
    copy_up(0).start()
    copy_up(1).start()
    esc[:, pl.ds(0, D)] = layer_norm(xb, hb, 0)

    diag = (lax.broadcasted_iota(jnp.int32, (SEQ, SEQ), 0)
            == lax.broadcasted_iota(jnp.int32, (SEQ, SEQ), 1))
    pos_row = jnp.broadcast_to(posb[...].astype(F32).reshape(1, SEQ), (SEQ, SEQ))
    pos_col = jnp.sum(jnp.where(diag, pos_row, 0.0), axis=1, keepdims=True)
    angle = pos_col * freqb[...]
    cos, sin = jnp.cos(angle), jnp.sin(angle)
    hl = lax.broadcasted_iota(jnp.int32, (SEQ, HEAD_DIM), 1)
    keep = jnp.where(hl < ROT_DIM, cos, 1.0)
    from_right = jnp.where(hl < ROT_DIM // 2, -sin, 0.0)
    from_left = jnp.where((hl >= ROT_DIM // 2) & (hl < ROT_DIM), sin, 0.0)
    keep = jnp.concatenate([keep, keep], axis=0)
    from_right = jnp.concatenate([from_right, from_right], axis=0)
    from_left = jnp.concatenate([from_left, from_left], axis=0)

    def proj(u):
        return jnp.dot(hb[...], wbuf[pl.ds(u * UNIT, 2 * UNIT), :], preferred_element_type=F32)

    def rope(v):
        u = v.astype(BF16).astype(F32)
        r = pltpu.roll(u, HEAD_DIM - ROT_DIM // 2, 1)
        l = pltpu.roll(u, ROT_DIM // 2, 1)
        return (u * keep + r * from_right + l * from_left).astype(BF16)

    arrive(6, 4, 7)
    copy_up(2).start()
    copy_up(3).start()
    kk = proj(6)
    vv = proj(8)
    for g in range(4):
        ks[pl.ds(g * ROWS, ROWS), :] = rope(kk[:, g * HEAD_DIM:(g + 1) * HEAD_DIM])
    vs[...] = vv.astype(BF16)

    row = lax.broadcasted_iota(jnp.int32, (3 * ROWS, ROWS), 0) & (ROWS - 1)
    col = lax.broadcasted_iota(jnp.int32, (3 * ROWS, ROWS), 1)
    same = (row >= SEQ) == (col >= SEQ)
    allowed = same & (col <= row)
    blocked = jnp.where(same, F32(-1e30), F32(-jnp.inf))
    lane = lax.broadcasted_iota(jnp.int32, (1, ROWS), 1)

    def attention(g, head_sq):
        q = qs[pl.ds(g * 3 * ROWS, 3 * ROWS), :]
        k = ks[pl.ds(g * ROWS, ROWS), :]
        v = vs[:, g * HEAD_DIM:(g + 1) * HEAD_DIM]
        s = lax.dot_general(q, k, (((1,), (1,)), ((), ())), preferred_element_type=F32) * HEAD_DIM ** -0.5
        s = jnp.where(allowed, s, blocked)
        e = jnp.exp(s - jnp.max(s, axis=-1, keepdims=True))
        p = (e / jnp.sum(e, axis=-1, keepdims=True)).astype(BF16)
        o = jnp.dot(p, v, preferred_element_type=F32).astype(BF16)
        of = o.astype(F32)
        norm = jnp.sqrt(jnp.sum(of * of, axis=-1, keepdims=True))
        for j in range(3):
            i = 3 * g + j
            at[:, i * HEAD_DIM:(i + 1) * HEAD_DIM] = o[j * ROWS:(j + 1) * ROWS, :]
            m0 = jnp.sum(norm[j * ROWS:j * ROWS + SEQ], axis=0, keepdims=True) * (1.0 / SEQ)
            m1 = jnp.sum(norm[j * ROWS + SEQ:(j + 1) * ROWS], axis=0, keepdims=True) * (1.0 / SEQ)
            head_sq = head_sq + jnp.where(lane == i, m0 * m0 + m1 * m1, 0.0)
        return head_sq

    def query(c):
        qq = proj(2 * c)
        for j in range(4):
            qs[pl.ds((4 * c + j) * ROWS, ROWS), :] = rope(qq[:, j * HEAD_DIM:(j + 1) * HEAD_DIM])

    head_sq = jnp.zeros((1, ROWS), F32)
    arrive(0, 4, 8)
    copy_up(4).start()
    copy_up(5).start()
    query(0)
    query(1)
    head_sq = attention(0, head_sq)
    head_sq = attention(1, head_sq)
    arrive(4, 2, 9)
    copy_up(6).start()
    copy_up(7).start()
    for r0, n, i in UP_LAST:
        copy_up_last(r0, n, i).start()
    query(2)
    head_sq = attention(2, head_sq)
    head_sq = attention(3, head_sq)
    esc[:, pl.ds(D, 128)] = head_sq

    def send(c):
        return pltpu.make_async_remote_copy(
            src_ref=xsend.at[c], dst_ref=xrecv.at[c], send_sem=tp_send, recv_sem=tp_recv.at[TP_SEM[c]],
            device_id={"tp": partner}, device_id_type=MESH)

    def receive(c, n):
        part = pl.ds(c, n)
        pltpu.make_async_remote_copy(
            src_ref=xsend.at[part], dst_ref=xrecv.at[part], send_sem=tp_send, recv_sem=tp_recv.at[TP_SEM[c]],
            device_id={"tp": partner}, device_id_type=MESH).wait_recv()

    pl.semaphore_wait(barrier, n_peers)

    for part in range(2):
        arrive(O_U + 3 * part, 3, 10 + part)
        if part == 0:
            copy_dn(0).start()
            copy_dn(1).start()
        else:
            copy_dn(2).start()
        for c in range(3 * part, 3 * part + 3):
            xsend[c] = jnp.dot(at[...], wbuf[pl.ds((O_U + c) * UNIT, UNIT), :], preferred_element_type=F32)
            send(c).start()
        if part == 1:
            copy_dn(3).start()
    for part in range(2):
        receive(3 * part, 3)
        for c in range(3 * part, 3 * part + 3):
            cs = pl.ds(c * CW, CW)
            xm[:, cs] = (xb[:, cs].astype(F32) + (xsend[c] + xrecv[c])).astype(BF16)

    esc[:, pl.ds(0, D)] = esc[:, pl.ds(0, D)] + layer_norm(xm, hb, 1)

    def ar_copy(buf, group, phase, src, k):
        return pltpu.make_async_remote_copy(
            src_ref=src, dst_ref=src, send_sem=ar_send.at[group], recv_sem=ar_recv.at[group, phase],
            device_id={"dp": peer(phase, k)}, device_id_type=MESH)

    def ar_start(buf, group, phase, value):
        buf[phase, place[phase]] = value
        for k in range(1, group_size[phase]):
            ar_copy(buf, group, phase, buf.at[phase, place[phase]], k).start()

    def ar_finish(buf, group, phase):
        ar_copy(buf, group, phase, buf.at[phase, pl.ds(0, group_size[phase] - 1)], 1).wait_recv()
        total = buf[phase, 0]
        for j in range(1, group_size[phase]):
            total = total + buf[phase, j]
        return total

    def ar_sent(buf, group):
        ar_copy(buf, group, 0, buf.at[:, pl.ds(0, group_size[0] - 1)], 1).wait_send()

    def e_finish():
        total = jnp.sqrt(ar_finish(are, 0, 1))
        fe_ref[...] = total[:, :D].reshape(D)
        fh_ref[...] = total[:, D:].reshape(128)[:12]

    def na_finish():
        fn_ref[pl.ds(0, NA)] = jnp.sqrt(ar_finish(arn, 1, 1)).reshape(NA)

    NB = FL - NA

    def cross_copy(phase, src, dst, k):
        return pltpu.make_async_remote_copy(
            src_ref=src, dst_ref=dst, send_sem=ar_send.at[3], recv_sem=ar_recv.at[3, phase],
            device_id={"dp": peer(phase, k) if k else dp, "tp": partner}, device_id_type=MESH)

    def cross_start(phase, src):
        for k in range(group_size[phase]):
            cross_copy(phase, src, ars.at[phase, place[phase]], k).start()

    def cross_finish(phase):
        cross_copy(phase, ars.at[phase], ars.at[phase], 0).wait_recv()
        total = ars[phase, 0]
        for j in range(1, group_size[phase]):
            total = total + ars[phase, j]
        return total

    def nb_start():
        @pl.when(tp == 0)
        def _():
            cross_start(0, nsc.at[:, pl.ds(NA, NB)])

        @pl.when(tp == 1)
        def _():
            ar_start(arm, 2, 0, nsc[:, pl.ds(NA, NB)])

    def nb_middle():
        @pl.when(tp == 1)
        def _():
            ar_start(arm, 2, 1, ar_finish(arm, 2, 0))
            stage[...] = cross_finish(0)
            cross_start(1, stage)

    def nb_finish():
        @pl.when(tp == 0)
        def _():
            fn_ref[pl.ds(NA, NB)] = jnp.sqrt(cross_finish(1)).reshape(NB)

        @pl.when(tp == 1)
        def _():
            fn_ref[pl.ds(NA, NB)] = jnp.sqrt(ar_finish(arm, 2, 1)).reshape(NB)
            ar_sent(arm, 2)
        cross_copy(0, ars.at[0], ars.at[0], 0).wait_send()

    ar_start(are, 0, 0, esc[...])

    def up_score(c, u):
        r = jnp.maximum(u, 0.0)
        a = r * r
        cs = pl.ds(c * CW, CW)
        act[:, cs] = a.astype(BF16)
        m0 = jnp.sum(a[:SEQ], axis=0, keepdims=True) * (1.0 / SEQ)
        m1 = jnp.sum(a[SEQ:], axis=0, keepdims=True) * (1.0 / SEQ)
        nsc[:, cs] = m0 * m0 + m1 * m1

    def up_dot(c):
        return jnp.dot(hb[...], wbuf[pl.ds((UP_U + 2 * c) * UNIT, 2 * UNIT), :], preferred_element_type=F32)

    for i, chunks in enumerate(((0, 1, 2), (3, 4), (5,), (6,), (7,))):
        arrive(UP_U + 2 * chunks[0], 2 * len(chunks), UP_SEM[chunks[0]])
        if i == 1:
            copy_dn(4).start()
            copy_dn(5, 0, 1).start()
        elif i == 3:
            copy_dn(5, 1, 1).start()
            copy_dn(5, 2, 1).start()
        for c in chunks:
            up_score(c, up_dot(c))
        if i == 2:
            ar_start(arn, 1, 0, nsc[:, pl.ds(0, NA)])
    u = None
    for r0, n, i in UP_LAST:
        copy_up_last(r0, n, i).wait()
        part = jnp.dot(hb[:, pl.ds(r0, n)], wbuf[pl.ds(r0, n), :], preferred_element_type=F32)
        u = part if u is None else u + part
    up_score(N_UP - 1, u)
    nb_start()

    def finish_d(first, n):
        receive(N_O + first, n)
        for c in range(first, first + n):
            cs = pl.ds(c * CW, CW)
            y_ref[:, cs] = (xm[:, cs].astype(F32) + (xsend[N_O + c] + xrecv[N_O + c])).astype(BF16)

    hooks = {
        0: lambda: ar_start(are, 0, 1, ar_finish(are, 0, 0)),
        1: lambda: ar_start(arn, 1, 1, ar_finish(arn, 1, 0)),
        2: nb_middle,
        5: lambda: (e_finish(), na_finish()),
    }

    for c in range(N_DN):
        acc = None
        n = DN_U if c < N_DN - 1 else 1
        for u in range(0, DN_U, n):
            copy_dn(c, u, n).wait()
            part = jnp.dot(act[:, pl.ds(u * UNIT, n * UNIT)],
                           wbuf[pl.ds((DN_B + DN_U * c + u) * UNIT, n * UNIT), :],
                           preferred_element_type=F32)
            acc = part if acc is None else acc + part
        xsend[N_O + c] = acc
        send(N_O + c).start()
        if c in (3, 5):
            finish_d(c - 3, 2)
        if c in hooks:
            hooks[c]()
    finish_d(N_DN - 2, 1)
    finish_d(N_DN - 1, 1)
    nb_finish()

    pltpu.make_async_remote_copy(
        src_ref=xsend, dst_ref=xrecv, send_sem=tp_send, recv_sem=tp_recv.at[0],
        device_id={"tp": partner}, device_id_type=MESH).wait_send()
    ar_sent(are, 0)
    ar_sent(arn, 1)


def writer(y, fn, fh, fe, y_out, fn_out, fh_out, fe_out, sem):
    copies = [pltpu.make_async_copy(a, b, sem.at[i])
              for i, (a, b) in enumerate(((y, y_out), (fn, fn_out), (fh, fh_out), (fe, fe_out)))]
    for c in copies:
        c.start()
    for c in copies:
        c.wait()


def solution(mesh):
    dims = (4, 4, 4)

    def local_layer(hidden, positions, ln1_gain, ln1_bias, w_q, w_k, w_v, w_o, ln2_gain, ln2_bias, w_up, w_down):
        hbm = pl.BlockSpec(memory_space=pltpu.HBM)
        vmem = pl.BlockSpec(memory_space=pltpu.VMEM)
        y, fn, fh, fe = pl.pallas_call(
            functools.partial(body, dims),
            out_shape=(
                pltpu.VMEM((ROWS, D), BF16),
                pltpu.VMEM((FL,), F32),
                pltpu.VMEM((12,), F32),
                pltpu.VMEM((D,), F32),
            ),
            in_specs=[hbm] * 13,
            out_specs=(vmem, vmem, vmem, vmem),
            scratch_shapes=[
                pltpu.VMEM((NU * UNIT, CW), BF16),
                pltpu.VMEM((D,), BF16),
                pltpu.VMEM((D,), BF16),
                pltpu.VMEM((D,), BF16),
                pltpu.VMEM((D,), BF16),
                pltpu.VMEM((SEQ,), jnp.int32),
                pltpu.VMEM((1, HEAD_DIM), F32),
                pltpu.VMEM((ROWS, D), BF16),
                pltpu.VMEM((ROWS, D), BF16),
                pltpu.VMEM((ROWS, D), BF16),
                pltpu.VMEM((12 * ROWS, HEAD_DIM), BF16),
                pltpu.VMEM((4 * ROWS, HEAD_DIM), BF16),
                pltpu.VMEM((ROWS, KL), BF16),
                pltpu.VMEM((ROWS, QL), BF16),
                pltpu.VMEM((ROWS, FL), BF16),
                pltpu.VMEM((N_O + N_DN, ROWS, CW), F32),
                pltpu.VMEM((N_O + N_DN, ROWS, CW), F32),
                pltpu.VMEM((1, FL), F32),
                pltpu.VMEM((1, EH), F32),
                pltpu.VMEM((2, 8, 1, EH), F32),
                pltpu.VMEM((2, 8, 1, NA), F32),
                pltpu.VMEM((2, 8, 1, FL - NA), F32),
                pltpu.VMEM((2, 8, 1, FL - NA), F32),
                pltpu.VMEM((1, FL - NA), F32),
                pltpu.SemaphoreType.DMA((12,)),
                pltpu.SemaphoreType.DMA,
                pltpu.SemaphoreType.DMA((6,)),
                pltpu.SemaphoreType.DMA((4,)),
                pltpu.SemaphoreType.DMA((4, 2)),
            ],
            compiler_params=pltpu.CompilerParams(
                collective_id=0, has_side_effects=True, vmem_limit_bytes=62 * 2**20),
            name="layer",
        )(hidden.reshape(ROWS, D), positions, jnp.asarray(inv_freq_row()), ln1_gain, ln1_bias, ln2_gain, ln2_bias,
          w_q, w_k, w_v, w_o, w_up, w_down)
        held = [pltpu.with_memory_space_constraint(v, pltpu.VMEM) for v in (y, fn, fh, fe)]
        y, fn, fh, fe = pl.pallas_call(
            writer,
            out_shape=tuple(jax.ShapeDtypeStruct(v.shape, v.dtype) for v in held),
            in_specs=[vmem] * 4,
            out_specs=(hbm,) * 4,
            scratch_shapes=[pltpu.SemaphoreType.DMA((4,))],
            name="writer",
        )(*held)
        return y.reshape(hidden.shape), fn, fh, fe

    weight_col = P(None, "tp")
    weight_row = P("tp", None)
    return jax.shard_map(
        local_layer,
        mesh=mesh,
        in_specs=(P("dp"), P(), P(), P(), weight_col, weight_col, weight_col, weight_row, P(), P(), weight_col, weight_row),
        out_specs=(P("dp"), P("tp"), P("tp"), P()),
        check_vma=False,
    )
```

```python
import functools

import jax
import jax.numpy as jnp
import numpy as np
from jax import lax
from jax.experimental import pallas as pl
from jax.experimental.pallas import tpu as pltpu
from jax.sharding import PartitionSpec as P

HEAD_DIM = 128
ROT_DIM = 64
ROPE_BASE = 10000.0
LN_EPS = 1e-5
MESH = pl.DeviceIdType.MESH
F32 = jnp.float32
BF16 = jnp.bfloat16

SEQ = 64
ROWS = 128
D = 3072
QL = 1536
KL = 512
FL = 4608
CW = 512
UNIT = 1536
NU = 32
N_O = D // CW
N_UP = FL // CW
NA = 5 * CW
N_DN = D // CW
DN_U = FL // UNIT
EH = D + 128

O_U = 10
UP_U = 16
DN_B = 2
TP_SEM = (0, 0, 0, 1, 1, 1, 2, 2, 3, 3, 4, 5)
UP_SEM = (0, 0, 0, 1, 1, 2, 2, 3)
UP_LAST = ((0, 2048, 5), (2048, 1024, 6))
DN_SEM = (7, 8, 9, 10, 11, 0, 1, 2)


def inv_freq_row():
    half = ROT_DIM // 2
    freq = ROPE_BASE ** (-2.0 * np.arange(half, dtype=np.float64) / ROT_DIM)
    return np.concatenate([freq, freq, np.zeros(HEAD_DIM - ROT_DIM)])[None, :].astype(np.float32)


def body(sizes, x_hbm, pos_hbm, freq_hbm, g1, b1, g2, b2, wq, wk, wv, wo, wup, wdn,
         y_ref, fn_ref, fh_ref, fe_ref,
         wbuf, ln0, ln1, ln2, ln3, posb, freqb, xb, hb, xm, qs, ks, vs, at, act, ub, xsend, xrecv,
         nsc, esc, are, arn, arm, ars, stage,
         sem, tp_send, tp_recv, ar_send, ar_recv):
    dims = sizes
    tp = lax.axis_index("tp")
    dp = lax.axis_index("dp")
    sz, sy, sx = dims
    ix = lax.rem(dp, sx)
    iy = lax.rem(lax.div(dp, sx), sy)
    iz = lax.div(dp, sx * sy)
    partner = 1 - tp

    def peer(phase, k):
        step, flip = k // 2, k % 2
        if phase == 0:
            to_x, to_z = lax.rem(ix + step, sx), iz
            to_y = sy - 1 - iy if flip else iy
        else:
            to_x, to_z = ix, lax.rem(iz + step, sz)
            to_y = iy + 1 - 2 * lax.rem(iy, 2) if flip else iy
        return to_x + sx * (to_y + sy * to_z)

    place = (2 * ix + lax.div(iy, 2), 2 * iz + lax.rem(lax.div(iy + 1, 2), 2))
    group_size = (2 * sx, 2 * sz)

    def slot(u, n):
        return wbuf.at[pl.ds(u * UNIT, n * UNIT), :]

    def cols(ref, c):
        return ref.at[:, pl.ds(c * CW, CW)]

    def arrive(u, n, s):
        pltpu.make_async_copy(slot(u, n), slot(u, n), sem.at[s]).wait()

    def copy_k():
        return pltpu.make_async_copy(wk, slot(6, 2), sem.at[7])

    def copy_v():
        return pltpu.make_async_copy(wv, slot(8, 2), sem.at[7])

    def copy_q(c):
        return pltpu.make_async_copy(cols(wq, c), slot(2 * c, 2), sem.at[8 + c // 2])

    def copy_o(c):
        return pltpu.make_async_copy(cols(wo, c), slot(O_U + c, 1), sem.at[10 + c // 3])

    def copy_up(c):
        return pltpu.make_async_copy(cols(wup, c), slot(UP_U + 2 * c, 2), sem.at[UP_SEM[c]])

    def copy_up_last(r0, n, i):
        return pltpu.make_async_copy(wup.at[pl.ds(r0, n), pl.ds((N_UP - 1) * CW, CW)],
                                     wbuf.at[pl.ds(r0, n), :], sem.at[i])

    def copy_dn(c, u=0, n=DN_U):
        return pltpu.make_async_copy(
            wdn.at[pl.ds(u * UNIT, n * UNIT), pl.ds(c * CW, CW)],
            slot(DN_B + DN_U * c + u, n), sem.at[DN_SEM[c + u]])

    def copy_x():
        return pltpu.make_async_copy(x_hbm, xb, sem.at[0])

    lnb = (ln0, ln1, ln2, ln3)
    small = [pltpu.make_async_copy(r, lnb[i], sem.at[1 + i]) for i, r in enumerate((g1, b1, g2, b2))]
    small.append(pltpu.make_async_copy(pos_hbm, posb, sem.at[5]))
    small.append(pltpu.make_async_copy(freq_hbm, freqb, sem.at[6]))

    barrier = pltpu.get_barrier_semaphore()
    greet = [{"tp": partner}]
    for phase in range(2):
        for k in range(1, group_size[phase]):
            greet.append({"dp": peer(phase, k)})
            greet.append({"dp": peer(phase, k), "tp": partner})
    first = [lambda: [copy_x().start()], lambda: [c.start() for c in small],
             lambda: [copy_k().start()], lambda: [copy_v().start()]]
    first += [lambda c=c: [copy_q(c).start()] for c in range(3)]
    first += [lambda c=c: [copy_o(c).start()] for c in range(N_O)]
    for i in range(max(len(first), len(greet))):
        if i < len(first):
            first[i]()
        if i < len(greet):
            pl.semaphore_signal(barrier, inc=1, device_id=greet[i], device_id_type=MESH)
    n_peers = len(greet)

    def layer_norm(src, dst, which):
        gain = 1.0 + lnb[2 * which][...].astype(F32).reshape(1, D)
        bias = lnb[2 * which + 1][...].astype(F32).reshape(1, D)
        for i in range(ROWS // 16):
            rows = pl.ds(i * 16, 16)
            v = src[rows, :].astype(F32)
            mean = jnp.mean(v, axis=-1, keepdims=True)
            cen = v - mean
            var = jnp.mean(cen * cen, axis=-1, keepdims=True)
            dst[rows, :] = (cen * lax.rsqrt(var + LN_EPS) * gain + bias).astype(BF16)

    def token_squares(src):
        total = None
        for b in range(ROWS // SEQ):
            acc = None
            for i in range(SEQ // 16):
                hf = src[pl.ds(b * SEQ + i * 16, 16), :].astype(F32)
                part = hf[:8] + hf[8:]
                acc = part if acc is None else acc + part
            mean_tok = jnp.sum(acc, axis=0, keepdims=True) * (1.0 / SEQ)
            sq = mean_tok * mean_tok
            total = sq if total is None else total + sq
        return total

    for c in small:
        c.wait()
    copy_x().wait()
    copy_up(0).start()
    copy_up(1).start()
    layer_norm(xb, hb, 0)

    diag = (lax.broadcasted_iota(jnp.int32, (SEQ, SEQ), 0)
            == lax.broadcasted_iota(jnp.int32, (SEQ, SEQ), 1))
    pos_row = jnp.broadcast_to(posb[...].astype(F32).reshape(1, SEQ), (SEQ, SEQ))
    pos_col = jnp.sum(jnp.where(diag, pos_row, 0.0), axis=1, keepdims=True)
    angle = pos_col * freqb[...]
    cos, sin = jnp.cos(angle), jnp.sin(angle)
    hl = lax.broadcasted_iota(jnp.int32, (SEQ, HEAD_DIM), 1)
    keep = jnp.where(hl < ROT_DIM, cos, 1.0)
    from_right = jnp.where(hl < ROT_DIM // 2, -sin, 0.0)
    from_left = jnp.where((hl >= ROT_DIM // 2) & (hl < ROT_DIM), sin, 0.0)
    keep = jnp.concatenate([keep, keep], axis=0)
    from_right = jnp.concatenate([from_right, from_right], axis=0)
    from_left = jnp.concatenate([from_left, from_left], axis=0)

    def proj(u):
        return jnp.dot(hb[...], wbuf[pl.ds(u * UNIT, 2 * UNIT), :], preferred_element_type=F32)

    def rope(v):
        u = v.astype(BF16).astype(F32)
        r = pltpu.roll(u, HEAD_DIM - ROT_DIM // 2, 1)
        l = pltpu.roll(u, ROT_DIM // 2, 1)
        return (u * keep + r * from_right + l * from_left).astype(BF16)

    arrive(6, 4, 7)
    copy_up(2).start()
    copy_up(3).start()
    kk = proj(6)
    vv = proj(8)
    for g in range(4):
        ks[pl.ds(g * ROWS, ROWS), :] = rope(kk[:, g * HEAD_DIM:(g + 1) * HEAD_DIM])
    vs[...] = vv.astype(BF16)
    esc[:, pl.ds(0, D)] = token_squares(hb)

    row = lax.broadcasted_iota(jnp.int32, (3 * ROWS, ROWS), 0) & (ROWS - 1)
    col = lax.broadcasted_iota(jnp.int32, (3 * ROWS, ROWS), 1)
    same = (row >= SEQ) == (col >= SEQ)
    allowed = same & (col <= row)
    blocked = jnp.where(same, F32(-1e30), F32(-jnp.inf))
    lane = lax.broadcasted_iota(jnp.int32, (1, ROWS), 1)

    def attention(g, head_sq):
        q = qs[pl.ds(g * 3 * ROWS, 3 * ROWS), :]
        k = ks[pl.ds(g * ROWS, ROWS), :]
        v = vs[:, g * HEAD_DIM:(g + 1) * HEAD_DIM]
        s = lax.dot_general(q, k, (((1,), (1,)), ((), ())), preferred_element_type=F32) * HEAD_DIM ** -0.5
        s = jnp.where(allowed, s, blocked)
        e = jnp.exp(s - jnp.max(s, axis=-1, keepdims=True))
        p = (e / jnp.sum(e, axis=-1, keepdims=True)).astype(BF16)
        o = jnp.dot(p, v, preferred_element_type=F32).astype(BF16)
        of = o.astype(F32)
        norm = jnp.sqrt(jnp.sum(of * of, axis=-1, keepdims=True))
        for j in range(3):
            i = 3 * g + j
            at[:, i * HEAD_DIM:(i + 1) * HEAD_DIM] = o[j * ROWS:(j + 1) * ROWS, :]
            m0 = jnp.sum(norm[j * ROWS:j * ROWS + SEQ], axis=0, keepdims=True) * (1.0 / SEQ)
            m1 = jnp.sum(norm[j * ROWS + SEQ:(j + 1) * ROWS], axis=0, keepdims=True) * (1.0 / SEQ)
            head_sq = head_sq + jnp.where(lane == i, m0 * m0 + m1 * m1, 0.0)
        return head_sq

    def query(c):
        qq = proj(2 * c)
        for j in range(4):
            qs[pl.ds((4 * c + j) * ROWS, ROWS), :] = rope(qq[:, j * HEAD_DIM:(j + 1) * HEAD_DIM])

    head_sq = jnp.zeros((1, ROWS), F32)
    arrive(0, 4, 8)
    copy_up(4).start()
    copy_up(5).start()
    query(0)
    query(1)
    head_sq = attention(0, head_sq)
    head_sq = attention(1, head_sq)
    arrive(4, 2, 9)
    copy_up(6).start()
    copy_up(7).start()
    for r0, n, i in UP_LAST:
        copy_up_last(r0, n, i).start()
    query(2)
    head_sq = attention(2, head_sq)
    head_sq = attention(3, head_sq)
    esc[:, pl.ds(D, 128)] = head_sq

    def send(c):
        return pltpu.make_async_remote_copy(
            src_ref=xsend.at[c], dst_ref=xrecv.at[c], send_sem=tp_send, recv_sem=tp_recv.at[TP_SEM[c]],
            device_id={"tp": partner}, device_id_type=MESH)

    def receive(c, n):
        part = pl.ds(c, n)
        pltpu.make_async_remote_copy(
            src_ref=xsend.at[part], dst_ref=xrecv.at[part], send_sem=tp_send, recv_sem=tp_recv.at[TP_SEM[c]],
            device_id={"tp": partner}, device_id_type=MESH).wait_recv()

    pl.semaphore_wait(barrier, n_peers)

    for part in range(2):
        arrive(O_U + 3 * part, 3, 10 + part)
        if part == 0:
            copy_dn(0).start()
            copy_dn(1).start()
        else:
            copy_dn(2).start()
        for c in range(3 * part, 3 * part + 3):
            xsend[c] = jnp.dot(at[...], wbuf[pl.ds((O_U + c) * UNIT, UNIT), :], preferred_element_type=F32)
            send(c).start()
        if part == 1:
            copy_dn(3).start()
    for part in range(2):
        receive(3 * part, 3)
        for c in range(3 * part, 3 * part + 3):
            cs = pl.ds(c * CW, CW)
            xm[:, cs] = (xb[:, cs].astype(F32) + (xsend[c] + xrecv[c])).astype(BF16)

    layer_norm(xm, hb, 1)

    def ar_copy(buf, group, phase, src, k):
        return pltpu.make_async_remote_copy(
            src_ref=src, dst_ref=src, send_sem=ar_send.at[group], recv_sem=ar_recv.at[group, phase],
            device_id={"dp": peer(phase, k)}, device_id_type=MESH)

    def ar_start(buf, group, phase, value):
        buf[phase, place[phase]] = value
        for k in range(1, group_size[phase]):
            ar_copy(buf, group, phase, buf.at[phase, place[phase]], k).start()

    def ar_finish(buf, group, phase):
        ar_copy(buf, group, phase, buf.at[phase, pl.ds(0, group_size[phase] - 1)], 1).wait_recv()
        total = buf[phase, 0]
        for j in range(1, group_size[phase]):
            total = total + buf[phase, j]
        return total

    def ar_sent(buf, group):
        ar_copy(buf, group, 0, buf.at[:, pl.ds(0, group_size[0] - 1)], 1).wait_send()

    def e_finish():
        total = jnp.sqrt(ar_finish(are, 0, 1))
        fe_ref[...] = total[:, :D].reshape(D)
        fh_ref[...] = total[:, D:].reshape(128)[:12]

    def na_finish():
        fn_ref[pl.ds(0, NA)] = jnp.sqrt(ar_finish(arn, 1, 1)).reshape(NA)

    NB = FL - NA

    def cross_copy(phase, src, dst, k):
        return pltpu.make_async_remote_copy(
            src_ref=src, dst_ref=dst, send_sem=ar_send.at[3], recv_sem=ar_recv.at[3, phase],
            device_id={"dp": peer(phase, k) if k else dp, "tp": partner}, device_id_type=MESH)

    def cross_start(phase, src):
        for k in range(group_size[phase]):
            cross_copy(phase, src, ars.at[phase, place[phase]], k).start()

    def cross_finish(phase):
        cross_copy(phase, ars.at[phase], ars.at[phase], 0).wait_recv()
        total = ars[phase, 0]
        for j in range(1, group_size[phase]):
            total = total + ars[phase, j]
        return total

    def nb_start():
        @pl.when(tp == 0)
        def _():
            cross_start(0, nsc.at[:, pl.ds(NA, NB)])

        @pl.when(tp == 1)
        def _():
            ar_start(arm, 2, 0, nsc[:, pl.ds(NA, NB)])

    def nb_middle():
        @pl.when(tp == 1)
        def _():
            ar_start(arm, 2, 1, ar_finish(arm, 2, 0))
            stage[...] = cross_finish(0)
            cross_start(1, stage)

    def nb_finish():
        @pl.when(tp == 0)
        def _():
            fn_ref[pl.ds(NA, NB)] = jnp.sqrt(cross_finish(1)).reshape(NB)

        @pl.when(tp == 1)
        def _():
            fn_ref[pl.ds(NA, NB)] = jnp.sqrt(ar_finish(arm, 2, 1)).reshape(NB)
            ar_sent(arm, 2)
        cross_copy(0, ars.at[0], ars.at[0], 0).wait_send()


    def up_score(c, u):
        r = jnp.maximum(u, 0.0)
        a = r * r
        cs = pl.ds(c * CW, CW)
        act[:, cs] = a.astype(BF16)
        m0 = jnp.sum(a[:SEQ], axis=0, keepdims=True) * (1.0 / SEQ)
        m1 = jnp.sum(a[SEQ:], axis=0, keepdims=True) * (1.0 / SEQ)
        nsc[:, cs] = m0 * m0 + m1 * m1

    def up_dot(c):
        return jnp.dot(hb[...], wbuf[pl.ds((UP_U + 2 * c) * UNIT, 2 * UNIT), :], preferred_element_type=F32)

    for i, chunks in enumerate(((0, 1, 2), (3, 4), (5, 6), (7,))):
        arrive(UP_U + 2 * chunks[0], 2 * len(chunks), UP_SEM[chunks[0]])
        if i == 1:
            copy_dn(4).start()
            copy_dn(5, 0, 1).start()
        elif i == 3:
            copy_dn(5, 1, 1).start()
            copy_dn(5, 2, 1).start()
        for c in chunks:
            ub[c % 2] = up_dot(c)
            if c not in (0, 5):
                up_score(c - 1, ub[(c - 1) % 2])
        if i == 0:
            esc[:, pl.ds(0, D)] = esc[:, pl.ds(0, D)] + token_squares(hb)
            ar_start(are, 0, 0, esc[...])
        if i == 1:
            up_score(4, ub[0])
            ar_start(arn, 1, 0, nsc[:, pl.ds(0, NA)])
    for r0, n, i in UP_LAST:
        copy_up_last(r0, n, i).wait()
        part = jnp.dot(hb[:, pl.ds(r0, n)], wbuf[pl.ds(r0, n), :], preferred_element_type=F32)
        if r0 == 0:
            ub[(N_UP - 1) % 2] = part
            up_score(N_UP - 2, ub[(N_UP - 2) % 2])
        else:
            up_score(N_UP - 1, ub[(N_UP - 1) % 2] + part)
    nb_start()

    def finish_d(first, n):
        receive(N_O + first, n)
        for c in range(first, first + n):
            cs = pl.ds(c * CW, CW)
            y_ref[:, cs] = (xm[:, cs].astype(F32) + (xsend[N_O + c] + xrecv[N_O + c])).astype(BF16)

    hooks = {
        0: lambda: (ar_start(are, 0, 1, ar_finish(are, 0, 0)), ar_start(arn, 1, 1, ar_finish(arn, 1, 0))),
        2: nb_middle,
        5: lambda: (e_finish(), na_finish()),
    }

    for c in range(N_DN):
        acc = None
        n = DN_U if c < N_DN - 1 else 1
        for u in range(0, DN_U, n):
            copy_dn(c, u, n).wait()
            part = jnp.dot(act[:, pl.ds(u * UNIT, n * UNIT)],
                           wbuf[pl.ds((DN_B + DN_U * c + u) * UNIT, n * UNIT), :],
                           preferred_element_type=F32)
            acc = part if acc is None else acc + part
        xsend[N_O + c] = acc
        send(N_O + c).start()
        if c in (3, 5):
            finish_d(c - 3, 2)
        if c in hooks:
            hooks[c]()
    finish_d(N_DN - 2, 1)
    finish_d(N_DN - 1, 1)
    nb_finish()

    pltpu.make_async_remote_copy(
        src_ref=xsend, dst_ref=xrecv, send_sem=tp_send, recv_sem=tp_recv.at[0],
        device_id={"tp": partner}, device_id_type=MESH).wait_send()
    ar_sent(are, 0)
    ar_sent(arn, 1)


def writer(y, fn, fh, fe, y_out, fn_out, fh_out, fe_out, sem):
    copies = [pltpu.make_async_copy(a, b, sem.at[i])
              for i, (a, b) in enumerate(((y, y_out), (fn, fn_out), (fh, fh_out), (fe, fe_out)))]
    for c in copies:
        c.start()
    for c in copies:
        c.wait()


def solution(mesh):
    dims = (4, 4, 4)

    def local_layer(hidden, positions, ln1_gain, ln1_bias, w_q, w_k, w_v, w_o, ln2_gain, ln2_bias, w_up, w_down):
        hbm = pl.BlockSpec(memory_space=pltpu.HBM)
        vmem = pl.BlockSpec(memory_space=pltpu.VMEM)
        y, fn, fh, fe = pl.pallas_call(
            functools.partial(body, dims),
            out_shape=(
                pltpu.VMEM((ROWS, D), BF16),
                pltpu.VMEM((FL,), F32),
                pltpu.VMEM((12,), F32),
                pltpu.VMEM((D,), F32),
            ),
            in_specs=[hbm] * 13,
            out_specs=(vmem, vmem, vmem, vmem),
            scratch_shapes=[
                pltpu.VMEM((NU * UNIT, CW), BF16),
                pltpu.VMEM((D,), BF16),
                pltpu.VMEM((D,), BF16),
                pltpu.VMEM((D,), BF16),
                pltpu.VMEM((D,), BF16),
                pltpu.VMEM((SEQ,), jnp.int32),
                pltpu.VMEM((1, HEAD_DIM), F32),
                pltpu.VMEM((ROWS, D), BF16),
                pltpu.VMEM((ROWS, D), BF16),
                pltpu.VMEM((ROWS, D), BF16),
                pltpu.VMEM((12 * ROWS, HEAD_DIM), BF16),
                pltpu.VMEM((4 * ROWS, HEAD_DIM), BF16),
                pltpu.VMEM((ROWS, KL), BF16),
                pltpu.VMEM((ROWS, QL), BF16),
                pltpu.VMEM((ROWS, FL), BF16),
                pltpu.VMEM((2, ROWS, CW), F32),
                pltpu.VMEM((N_O + N_DN, ROWS, CW), F32),
                pltpu.VMEM((N_O + N_DN, ROWS, CW), F32),
                pltpu.VMEM((1, FL), F32),
                pltpu.VMEM((1, EH), F32),
                pltpu.VMEM((2, 8, 1, EH), F32),
                pltpu.VMEM((2, 8, 1, NA), F32),
                pltpu.VMEM((2, 8, 1, FL - NA), F32),
                pltpu.VMEM((2, 8, 1, FL - NA), F32),
                pltpu.VMEM((1, FL - NA), F32),
                pltpu.SemaphoreType.DMA((12,)),
                pltpu.SemaphoreType.DMA,
                pltpu.SemaphoreType.DMA((6,)),
                pltpu.SemaphoreType.DMA((4,)),
                pltpu.SemaphoreType.DMA((4, 2)),
            ],
            compiler_params=pltpu.CompilerParams(
                collective_id=0, has_side_effects=True, vmem_limit_bytes=62 * 2**20),
            name="layer",
        )(hidden.reshape(ROWS, D), positions, jnp.asarray(inv_freq_row()), ln1_gain, ln1_bias, ln2_gain, ln2_bias,
          w_q, w_k, w_v, w_o, w_up, w_down)
        held = [pltpu.with_memory_space_constraint(v, pltpu.VMEM) for v in (y, fn, fh, fe)]
        y, fn, fh, fe = pl.pallas_call(
            writer,
            out_shape=tuple(jax.ShapeDtypeStruct(v.shape, v.dtype) for v in held),
            in_specs=[vmem] * 4,
            out_specs=(hbm,) * 4,
            scratch_shapes=[pltpu.SemaphoreType.DMA((4,))],
            name="writer",
        )(*held)
        return y.reshape(hidden.shape), fn, fh, fe

    weight_col = P(None, "tp")
    weight_row = P("tp", None)
    return jax.shard_map(
        local_layer,
        mesh=mesh,
        in_specs=(P("dp"), P(), P(), P(), weight_col, weight_col, weight_col, weight_row, P(), P(), weight_col, weight_row),
        out_specs=(P("dp"), P("tp"), P("tp"), P()),
        check_vma=False,
    )
```

```python
import functools

import jax
import jax.numpy as jnp
import numpy as np
from jax import lax
from jax.experimental import pallas as pl
from jax.experimental.pallas import tpu as pltpu
from jax.sharding import PartitionSpec as P

HEAD_DIM = 128
ROT_DIM = 64
ROPE_BASE = 10000.0
LN_EPS = 1e-5
MESH = pl.DeviceIdType.MESH
F32 = jnp.float32
BF16 = jnp.bfloat16

SEQ = 64
ROWS = 128
D = 3072
QL = 1536
KL = 512
FL = 4608
CW = 512
UNIT = 1536
NU = 32
N_O = D // CW
N_UP = FL // CW
NA = 5 * CW
N_DN = D // CW
DN_U = FL // UNIT
EH = D + 128

O_U = 10
UP_U = 16
DN_B = 2
TP_SEM = (0, 0, 0, 1, 1, 1, 2, 2, 3, 3, 4, 5)
UP_SEM = (0, 0, 0, 1, 1, 2, 2, 3)
UP_LAST = ((0, 2048, 5), (2048, 1024, 6))
DN_SEM = (7, 8, 9, 10, 11, 0, 1, 2)


def inv_freq_row():
    half = ROT_DIM // 2
    freq = ROPE_BASE ** (-2.0 * np.arange(half, dtype=np.float64) / ROT_DIM)
    return np.concatenate([freq, freq, np.zeros(HEAD_DIM - ROT_DIM)])[None, :].astype(np.float32)


def body(sizes, x_hbm, pos_hbm, freq_hbm, g1, b1, g2, b2, wq, wk, wv, wo, wup, wdn,
         y_ref, fn_ref, fh_ref, fe_ref,
         wbuf, ln0, ln1, ln2, ln3, posb, freqb, xb, hb, xm, qs, ks, vs, at, act, ub, xsend, xrecv,
         nsc, esc, are, arn, arm, ars, stage,
         sem, tp_send, tp_recv, ar_send, ar_recv):
    dims = sizes
    tp = lax.axis_index("tp")
    dp = lax.axis_index("dp")
    sz, sy, sx = dims
    ix = lax.rem(dp, sx)
    iy = lax.rem(lax.div(dp, sx), sy)
    iz = lax.div(dp, sx * sy)
    partner = 1 - tp

    def peer(phase, k):
        step, flip = k // 2, k % 2
        if phase == 0:
            to_x, to_z = lax.rem(ix + step, sx), iz
            to_y = sy - 1 - iy if flip else iy
        else:
            to_x, to_z = ix, lax.rem(iz + step, sz)
            to_y = iy + 1 - 2 * lax.rem(iy, 2) if flip else iy
        return to_x + sx * (to_y + sy * to_z)

    place = (2 * ix + lax.div(iy, 2), 2 * iz + lax.rem(lax.div(iy + 1, 2), 2))
    group_size = (2 * sx, 2 * sz)

    def slot(u, n):
        return wbuf.at[pl.ds(u * UNIT, n * UNIT), :]

    def cols(ref, c):
        return ref.at[:, pl.ds(c * CW, CW)]

    def arrive(u, n, s):
        pltpu.make_async_copy(slot(u, n), slot(u, n), sem.at[s]).wait()

    def copy_k():
        return pltpu.make_async_copy(wk, slot(6, 2), sem.at[7])

    def copy_v():
        return pltpu.make_async_copy(wv, slot(8, 2), sem.at[7])

    def copy_q(c):
        return pltpu.make_async_copy(cols(wq, c), slot(2 * c, 2), sem.at[8 + c // 2])

    def copy_o(c):
        return pltpu.make_async_copy(cols(wo, c), slot(O_U + c, 1), sem.at[10 + c // 3])

    def copy_up(c):
        return pltpu.make_async_copy(cols(wup, c), slot(UP_U + 2 * c, 2), sem.at[UP_SEM[c]])

    def copy_up_last(r0, n, i):
        return pltpu.make_async_copy(wup.at[pl.ds(r0, n), pl.ds((N_UP - 1) * CW, CW)],
                                     wbuf.at[pl.ds(r0, n), :], sem.at[i])

    def copy_dn(c, u=0, n=DN_U):
        return pltpu.make_async_copy(
            wdn.at[pl.ds(u * UNIT, n * UNIT), pl.ds(c * CW, CW)],
            slot(DN_B + DN_U * c + u, n), sem.at[DN_SEM[c + u]])

    def copy_x():
        return pltpu.make_async_copy(x_hbm, xb, sem.at[0])

    lnb = (ln0, ln1, ln2, ln3)
    small = [pltpu.make_async_copy(r, lnb[i], sem.at[1 + i]) for i, r in enumerate((g1, b1, g2, b2))]
    small.append(pltpu.make_async_copy(pos_hbm, posb, sem.at[5]))
    small.append(pltpu.make_async_copy(freq_hbm, freqb, sem.at[6]))

    barrier = pltpu.get_barrier_semaphore()
    greet = [{"tp": partner}]
    for phase in range(2):
        for k in range(1, group_size[phase]):
            greet.append({"dp": peer(phase, k)})
            greet.append({"dp": peer(phase, k), "tp": partner})
    first = [lambda: [copy_x().start()], lambda: [c.start(priority=1) for c in small],
             lambda: [copy_k().start()], lambda: [copy_v().start()]]
    first += [lambda c=c: [copy_q(c).start()] for c in range(3)]
    first += [lambda c=c: [copy_o(c).start()] for c in range(N_O)]
    for i in range(max(len(first), len(greet))):
        if i < len(first):
            first[i]()
        if i < len(greet):
            pl.semaphore_signal(barrier, inc=1, device_id=greet[i], device_id_type=MESH)
    n_peers = len(greet)

    def layer_norm(src, dst, which):
        gain = 1.0 + lnb[2 * which][...].astype(F32).reshape(1, D)
        bias = lnb[2 * which + 1][...].astype(F32).reshape(1, D)
        for i in range(ROWS // 16):
            rows = pl.ds(i * 16, 16)
            v = src[rows, :].astype(F32)
            mean = jnp.mean(v, axis=-1, keepdims=True)
            cen = v - mean
            var = jnp.mean(cen * cen, axis=-1, keepdims=True)
            dst[rows, :] = (cen * lax.rsqrt(var + LN_EPS) * gain + bias).astype(BF16)

    def token_squares(src):
        total = None
        for b in range(ROWS // SEQ):
            acc = None
            for i in range(SEQ // 16):
                hf = src[pl.ds(b * SEQ + i * 16, 16), :].astype(F32)
                part = hf[:8] + hf[8:]
                acc = part if acc is None else acc + part
            mean_tok = jnp.sum(acc, axis=0, keepdims=True) * (1.0 / SEQ)
            sq = mean_tok * mean_tok
            total = sq if total is None else total + sq
        return total

    for c in small:
        c.wait()
    copy_x().wait()
    copy_up(0).start()
    copy_up(1).start()
    layer_norm(xb, hb, 0)

    diag = (lax.broadcasted_iota(jnp.int32, (SEQ, SEQ), 0)
            == lax.broadcasted_iota(jnp.int32, (SEQ, SEQ), 1))
    pos_row = jnp.broadcast_to(posb[...].astype(F32).reshape(1, SEQ), (SEQ, SEQ))
    pos_col = jnp.sum(jnp.where(diag, pos_row, 0.0), axis=1, keepdims=True)
    angle = pos_col * freqb[...]
    cos, sin = jnp.cos(angle), jnp.sin(angle)
    hl = lax.broadcasted_iota(jnp.int32, (SEQ, HEAD_DIM), 1)
    keep = jnp.where(hl < ROT_DIM, cos, 1.0)
    from_right = jnp.where(hl < ROT_DIM // 2, -sin, 0.0)
    from_left = jnp.where((hl >= ROT_DIM // 2) & (hl < ROT_DIM), sin, 0.0)
    keep = jnp.concatenate([keep, keep], axis=0)
    from_right = jnp.concatenate([from_right, from_right], axis=0)
    from_left = jnp.concatenate([from_left, from_left], axis=0)

    def proj(u):
        return jnp.dot(hb[...], wbuf[pl.ds(u * UNIT, 2 * UNIT), :], preferred_element_type=F32)

    def rope(v):
        u = v.astype(BF16).astype(F32)
        r = pltpu.roll(u, HEAD_DIM - ROT_DIM // 2, 1)
        l = pltpu.roll(u, ROT_DIM // 2, 1)
        return (u * keep + r * from_right + l * from_left).astype(BF16)

    arrive(6, 4, 7)
    copy_up(2).start()
    copy_up(3).start()
    kk = proj(6)
    vv = proj(8)
    for g in range(4):
        ks[pl.ds(g * ROWS, ROWS), :] = rope(kk[:, g * HEAD_DIM:(g + 1) * HEAD_DIM])
    vs[...] = vv.astype(BF16)
    esc[:, pl.ds(0, D)] = token_squares(hb)

    row = lax.broadcasted_iota(jnp.int32, (3 * ROWS, ROWS), 0) & (ROWS - 1)
    col = lax.broadcasted_iota(jnp.int32, (3 * ROWS, ROWS), 1)
    same = (row >= SEQ) == (col >= SEQ)
    allowed = same & (col <= row)
    blocked = jnp.where(same, F32(-1e30), F32(-jnp.inf))
    lane = lax.broadcasted_iota(jnp.int32, (1, ROWS), 1)

    def attention(g, head_sq):
        q = qs[pl.ds(g * 3 * ROWS, 3 * ROWS), :]
        k = ks[pl.ds(g * ROWS, ROWS), :]
        v = vs[:, g * HEAD_DIM:(g + 1) * HEAD_DIM]
        s = lax.dot_general(q, k, (((1,), (1,)), ((), ())), preferred_element_type=F32) * HEAD_DIM ** -0.5
        s = jnp.where(allowed, s, blocked)
        e = jnp.exp(s - jnp.max(s, axis=-1, keepdims=True))
        p = (e / jnp.sum(e, axis=-1, keepdims=True)).astype(BF16)
        o = jnp.dot(p, v, preferred_element_type=F32).astype(BF16)
        of = o.astype(F32)
        norm = jnp.sqrt(jnp.sum(of * of, axis=-1, keepdims=True))
        for j in range(3):
            i = 3 * g + j
            at[:, i * HEAD_DIM:(i + 1) * HEAD_DIM] = o[j * ROWS:(j + 1) * ROWS, :]
            m0 = jnp.sum(norm[j * ROWS:j * ROWS + SEQ], axis=0, keepdims=True) * (1.0 / SEQ)
            m1 = jnp.sum(norm[j * ROWS + SEQ:(j + 1) * ROWS], axis=0, keepdims=True) * (1.0 / SEQ)
            head_sq = head_sq + jnp.where(lane == i, m0 * m0 + m1 * m1, 0.0)
        return head_sq

    def query(c):
        qq = proj(2 * c)
        for j in range(4):
            qs[pl.ds((4 * c + j) * ROWS, ROWS), :] = rope(qq[:, j * HEAD_DIM:(j + 1) * HEAD_DIM])

    head_sq = jnp.zeros((1, ROWS), F32)
    arrive(0, 4, 8)
    copy_up(4).start()
    copy_up(5).start()
    query(0)
    query(1)
    head_sq = attention(0, head_sq)
    head_sq = attention(1, head_sq)
    arrive(4, 2, 9)
    copy_up(6).start()
    copy_up(7).start()
    for r0, n, i in UP_LAST:
        copy_up_last(r0, n, i).start()
    query(2)
    head_sq = attention(2, head_sq)
    head_sq = attention(3, head_sq)
    esc[:, pl.ds(D, 128)] = head_sq

    def send(c):
        return pltpu.make_async_remote_copy(
            src_ref=xsend.at[c], dst_ref=xrecv.at[c], send_sem=tp_send, recv_sem=tp_recv.at[TP_SEM[c]],
            device_id={"tp": partner}, device_id_type=MESH)

    def receive(c, n):
        part = pl.ds(c, n)
        pltpu.make_async_remote_copy(
            src_ref=xsend.at[part], dst_ref=xrecv.at[part], send_sem=tp_send, recv_sem=tp_recv.at[TP_SEM[c]],
            device_id={"tp": partner}, device_id_type=MESH).wait_recv()

    pl.semaphore_wait(barrier, n_peers)

    for part in range(2):
        arrive(O_U + 3 * part, 3, 10 + part)
        if part == 0:
            copy_dn(0).start()
            copy_dn(1).start()
        else:
            copy_dn(2).start()
        for c in range(3 * part, 3 * part + 3):
            xsend[c] = jnp.dot(at[...], wbuf[pl.ds((O_U + c) * UNIT, UNIT), :], preferred_element_type=F32)
            send(c).start()
        if part == 1:
            copy_dn(3).start()
    for part in range(2):
        receive(3 * part, 3)
        for c in range(3 * part, 3 * part + 3):
            cs = pl.ds(c * CW, CW)
            xm[:, cs] = (xb[:, cs].astype(F32) + (xsend[c] + xrecv[c])).astype(BF16)

    layer_norm(xm, hb, 1)

    def ar_copy(buf, group, phase, src, k):
        return pltpu.make_async_remote_copy(
            src_ref=src, dst_ref=src, send_sem=ar_send.at[group], recv_sem=ar_recv.at[group, phase],
            device_id={"dp": peer(phase, k)}, device_id_type=MESH)

    def ar_start(buf, group, phase, value):
        buf[phase, place[phase]] = value
        for k in range(1, group_size[phase]):
            ar_copy(buf, group, phase, buf.at[phase, place[phase]], k).start()

    def ar_finish(buf, group, phase):
        ar_copy(buf, group, phase, buf.at[phase, pl.ds(0, group_size[phase] - 1)], 1).wait_recv()
        total = buf[phase, 0]
        for j in range(1, group_size[phase]):
            total = total + buf[phase, j]
        return total

    def ar_sent(buf, group):
        ar_copy(buf, group, 0, buf.at[:, pl.ds(0, group_size[0] - 1)], 1).wait_send()

    def e_finish():
        total = jnp.sqrt(ar_finish(are, 0, 1))
        fe_ref[...] = total[:, :D].reshape(D)
        fh_ref[...] = total[:, D:].reshape(128)[:12]

    def na_finish():
        fn_ref[pl.ds(0, NA)] = jnp.sqrt(ar_finish(arn, 1, 1)).reshape(NA)

    NB = FL - NA

    def cross_copy(phase, src, dst, k):
        return pltpu.make_async_remote_copy(
            src_ref=src, dst_ref=dst, send_sem=ar_send.at[3], recv_sem=ar_recv.at[3, phase],
            device_id={"dp": peer(phase, k) if k else dp, "tp": partner}, device_id_type=MESH)

    def cross_start(phase, src):
        for k in range(group_size[phase]):
            cross_copy(phase, src, ars.at[phase, place[phase]], k).start()

    def cross_finish(phase):
        cross_copy(phase, ars.at[phase], ars.at[phase], 0).wait_recv()
        total = ars[phase, 0]
        for j in range(1, group_size[phase]):
            total = total + ars[phase, j]
        return total

    def nb_start():
        @pl.when(tp == 0)
        def _():
            cross_start(0, nsc.at[:, pl.ds(NA, NB)])

        @pl.when(tp == 1)
        def _():
            ar_start(arm, 2, 0, nsc[:, pl.ds(NA, NB)])

    def nb_middle():
        @pl.when(tp == 1)
        def _():
            ar_start(arm, 2, 1, ar_finish(arm, 2, 0))
            stage[...] = cross_finish(0)
            cross_start(1, stage)

    def nb_finish():
        @pl.when(tp == 0)
        def _():
            fn_ref[pl.ds(NA, NB)] = jnp.sqrt(cross_finish(1)).reshape(NB)

        @pl.when(tp == 1)
        def _():
            fn_ref[pl.ds(NA, NB)] = jnp.sqrt(ar_finish(arm, 2, 1)).reshape(NB)
            ar_sent(arm, 2)
        cross_copy(0, ars.at[0], ars.at[0], 0).wait_send()


    def up_score(c, u):
        r = jnp.maximum(u, 0.0)
        a = r * r
        cs = pl.ds(c * CW, CW)
        act[:, cs] = a.astype(BF16)
        m0 = jnp.sum(a[:SEQ], axis=0, keepdims=True) * (1.0 / SEQ)
        m1 = jnp.sum(a[SEQ:], axis=0, keepdims=True) * (1.0 / SEQ)
        nsc[:, cs] = m0 * m0 + m1 * m1

    def up_dot(c):
        return jnp.dot(hb[...], wbuf[pl.ds((UP_U + 2 * c) * UNIT, 2 * UNIT), :], preferred_element_type=F32)

    for i, chunks in enumerate(((0, 1, 2), (3, 4), (5, 6), (7,))):
        arrive(UP_U + 2 * chunks[0], 2 * len(chunks), UP_SEM[chunks[0]])
        if i == 1:
            copy_dn(4).start()
            copy_dn(5, 0, 1).start()
        elif i == 3:
            copy_dn(5, 1, 1).start()
            copy_dn(5, 2, 1).start()
        for c in chunks:
            ub[c % 2] = up_dot(c)
            if c not in (0, 5):
                up_score(c - 1, ub[(c - 1) % 2])
        if i == 0:
            esc[:, pl.ds(0, D)] = esc[:, pl.ds(0, D)] + token_squares(hb)
            ar_start(are, 0, 0, esc[...])
        if i == 1:
            up_score(4, ub[0])
            ar_start(arn, 1, 0, nsc[:, pl.ds(0, NA)])
    for r0, n, i in UP_LAST:
        copy_up_last(r0, n, i).wait()
        part = jnp.dot(hb[:, pl.ds(r0, n)], wbuf[pl.ds(r0, n), :], preferred_element_type=F32)
        if r0 == 0:
            ub[(N_UP - 1) % 2] = part
            up_score(N_UP - 2, ub[(N_UP - 2) % 2])
        else:
            up_score(N_UP - 1, ub[(N_UP - 1) % 2] + part)
    nb_start()

    def finish_d(first, n):
        receive(N_O + first, n)
        for c in range(first, first + n):
            cs = pl.ds(c * CW, CW)
            y_ref[:, cs] = (xm[:, cs].astype(F32) + (xsend[N_O + c] + xrecv[N_O + c])).astype(BF16)

    hooks = {
        0: lambda: (ar_start(are, 0, 1, ar_finish(are, 0, 0)), ar_start(arn, 1, 1, ar_finish(arn, 1, 0))),
        2: nb_middle,
        5: lambda: (e_finish(), na_finish()),
    }

    for c in range(N_DN):
        acc = None
        n = DN_U if c < N_DN - 1 else 1
        for u in range(0, DN_U, n):
            copy_dn(c, u, n).wait()
            part = jnp.dot(act[:, pl.ds(u * UNIT, n * UNIT)],
                           wbuf[pl.ds((DN_B + DN_U * c + u) * UNIT, n * UNIT), :],
                           preferred_element_type=F32)
            acc = part if acc is None else acc + part
        xsend[N_O + c] = acc
        send(N_O + c).start()
        if c in (3, 5):
            finish_d(c - 3, 2)
        if c in hooks:
            hooks[c]()
    finish_d(N_DN - 2, 1)
    finish_d(N_DN - 1, 1)
    nb_finish()

    pltpu.make_async_remote_copy(
        src_ref=xsend, dst_ref=xrecv, send_sem=tp_send, recv_sem=tp_recv.at[0],
        device_id={"tp": partner}, device_id_type=MESH).wait_send()
    ar_sent(are, 0)
    ar_sent(arn, 1)


def writer(y, fn, fh, fe, y_out, fn_out, fh_out, fe_out, sem):
    copies = [pltpu.make_async_copy(a, b, sem.at[i])
              for i, (a, b) in enumerate(((y, y_out), (fn, fn_out), (fh, fh_out), (fe, fe_out)))]
    for c in copies:
        c.start()
    for c in copies:
        c.wait()


def solution(mesh):
    dims = (4, 4, 4)

    def local_layer(hidden, positions, ln1_gain, ln1_bias, w_q, w_k, w_v, w_o, ln2_gain, ln2_bias, w_up, w_down):
        hbm = pl.BlockSpec(memory_space=pltpu.HBM)
        vmem = pl.BlockSpec(memory_space=pltpu.VMEM)
        y, fn, fh, fe = pl.pallas_call(
            functools.partial(body, dims),
            out_shape=(
                pltpu.VMEM((ROWS, D), BF16),
                pltpu.VMEM((FL,), F32),
                pltpu.VMEM((12,), F32),
                pltpu.VMEM((D,), F32),
            ),
            in_specs=[hbm] * 13,
            out_specs=(vmem, vmem, vmem, vmem),
            scratch_shapes=[
                pltpu.VMEM((NU * UNIT, CW), BF16),
                pltpu.VMEM((D,), BF16),
                pltpu.VMEM((D,), BF16),
                pltpu.VMEM((D,), BF16),
                pltpu.VMEM((D,), BF16),
                pltpu.VMEM((SEQ,), jnp.int32),
                pltpu.VMEM((1, HEAD_DIM), F32),
                pltpu.VMEM((ROWS, D), BF16),
                pltpu.VMEM((ROWS, D), BF16),
                pltpu.VMEM((ROWS, D), BF16),
                pltpu.VMEM((12 * ROWS, HEAD_DIM), BF16),
                pltpu.VMEM((4 * ROWS, HEAD_DIM), BF16),
                pltpu.VMEM((ROWS, KL), BF16),
                pltpu.VMEM((ROWS, QL), BF16),
                pltpu.VMEM((ROWS, FL), BF16),
                pltpu.VMEM((2, ROWS, CW), F32),
                pltpu.VMEM((N_O + N_DN, ROWS, CW), F32),
                pltpu.VMEM((N_O + N_DN, ROWS, CW), F32),
                pltpu.VMEM((1, FL), F32),
                pltpu.VMEM((1, EH), F32),
                pltpu.VMEM((2, 8, 1, EH), F32),
                pltpu.VMEM((2, 8, 1, NA), F32),
                pltpu.VMEM((2, 8, 1, FL - NA), F32),
                pltpu.VMEM((2, 8, 1, FL - NA), F32),
                pltpu.VMEM((1, FL - NA), F32),
                pltpu.SemaphoreType.DMA((12,)),
                pltpu.SemaphoreType.DMA,
                pltpu.SemaphoreType.DMA((6,)),
                pltpu.SemaphoreType.DMA((4,)),
                pltpu.SemaphoreType.DMA((4, 2)),
            ],
            compiler_params=pltpu.CompilerParams(
                collective_id=0, has_side_effects=True, vmem_limit_bytes=62 * 2**20),
            name="layer",
        )(hidden.reshape(ROWS, D), positions, jnp.asarray(inv_freq_row()), ln1_gain, ln1_bias, ln2_gain, ln2_bias,
          w_q, w_k, w_v, w_o, w_up, w_down)
        held = [pltpu.with_memory_space_constraint(v, pltpu.VMEM) for v in (y, fn, fh, fe)]
        y, fn, fh, fe = pl.pallas_call(
            writer,
            out_shape=tuple(jax.ShapeDtypeStruct(v.shape, v.dtype) for v in held),
            in_specs=[vmem] * 4,
            out_specs=(hbm,) * 4,
            scratch_shapes=[pltpu.SemaphoreType.DMA((4,))],
            name="writer",
        )(*held)
        return y.reshape(hidden.shape), fn, fh, fe

    weight_col = P(None, "tp")
    weight_row = P("tp", None)
    return jax.shard_map(
        local_layer,
        mesh=mesh,
        in_specs=(P("dp"), P(), P(), P(), weight_col, weight_col, weight_col, weight_row, P(), P(), weight_col, weight_row),
        out_specs=(P("dp"), P("tp"), P("tp"), P()),
        check_vma=False,
    )
```

```python
import functools

import jax
import jax.numpy as jnp
import numpy as np
from jax import lax
from jax.experimental import pallas as pl
from jax.experimental.pallas import tpu as pltpu
from jax.sharding import PartitionSpec as P

HEAD_DIM = 128
ROT_DIM = 64
ROPE_BASE = 10000.0
LN_EPS = 1e-5
MESH = pl.DeviceIdType.MESH
F32 = jnp.float32
BF16 = jnp.bfloat16

SEQ = 64
ROWS = 128
D = 3072
QL = 1536
KL = 512
FL = 4608
CW = 512
UNIT = 1536
NU = 32
N_O = D // CW
N_UP = FL // CW
NA = 5 * CW
N_DN = D // CW
DN_U = FL // UNIT
EH = D + 128

O_U = 10
UP_U = 16
DN_B = 2
TP_SEM = (0, 0, 0, 1, 1, 1, 2, 2, 3, 3, 4, 5)
UP_SEM = (0, 0, 0, 1, 1, 2, 2, 3)
UP_LAST = ((0, 2048, 5), (2048, 1024, 6))
DN_SEM = (7, 8, 9, 10, 11, 0, 1, 2)


def inv_freq_row():
    half = ROT_DIM // 2
    freq = ROPE_BASE ** (-2.0 * np.arange(half, dtype=np.float64) / ROT_DIM)
    return np.concatenate([freq, freq, np.zeros(HEAD_DIM - ROT_DIM)])[None, :].astype(np.float32)


def body(sizes, x_hbm, pos_hbm, freq_hbm, g1, b1, g2, b2, wq, wk, wv, wo, wup, wdn,
         y_ref, fn_ref, fh_ref, fe_ref,
         wbuf, ln0, ln1, ln2, ln3, posb, freqb, xb, hb, xm, qs, ks, vs, at, act, ub, xsend, xrecv,
         nsc, esc, are, arn, arm, ars, stage,
         sem, tp_send, tp_recv, ar_send, ar_recv):
    dims = sizes
    tp = lax.axis_index("tp")
    dp = lax.axis_index("dp")
    sz, sy, sx = dims
    ix = lax.rem(dp, sx)
    iy = lax.rem(lax.div(dp, sx), sy)
    iz = lax.div(dp, sx * sy)
    partner = 1 - tp

    def peer(phase, k):
        step, flip = k // 2, k % 2
        if phase == 0:
            to_x, to_z = lax.rem(ix + step, sx), iz
            to_y = sy - 1 - iy if flip else iy
        else:
            to_x, to_z = ix, lax.rem(iz + step, sz)
            to_y = iy + 1 - 2 * lax.rem(iy, 2) if flip else iy
        return to_x + sx * (to_y + sy * to_z)

    place = (2 * ix + lax.div(iy, 2), 2 * iz + lax.rem(lax.div(iy + 1, 2), 2))
    group_size = (2 * sx, 2 * sz)

    def slot(u, n):
        return wbuf.at[pl.ds(u * UNIT, n * UNIT), :]

    def cols(ref, c):
        return ref.at[:, pl.ds(c * CW, CW)]

    def arrive(u, n, s):
        pltpu.make_async_copy(slot(u, n), slot(u, n), sem.at[s]).wait()

    def copy_k():
        return pltpu.make_async_copy(wk, slot(6, 2), sem.at[7])

    def copy_v():
        return pltpu.make_async_copy(wv, slot(8, 2), sem.at[7])

    def copy_q(c):
        return pltpu.make_async_copy(cols(wq, c), slot(2 * c, 2), sem.at[8 + c // 2])

    def copy_o(c):
        return pltpu.make_async_copy(cols(wo, c), slot(O_U + c, 1), sem.at[10 + c // 3])

    def copy_up(c):
        return pltpu.make_async_copy(cols(wup, c), slot(UP_U + 2 * c, 2), sem.at[UP_SEM[c]])

    def copy_up_last(r0, n, i):
        return pltpu.make_async_copy(wup.at[pl.ds(r0, n), pl.ds((N_UP - 1) * CW, CW)],
                                     wbuf.at[pl.ds(r0, n), :], sem.at[i])

    def copy_dn(c, u=0, n=DN_U):
        return pltpu.make_async_copy(
            wdn.at[pl.ds(u * UNIT, n * UNIT), pl.ds(c * CW, CW)],
            slot(DN_B + DN_U * c + u, n), sem.at[DN_SEM[c + u]])

    def copy_x():
        return pltpu.make_async_copy(x_hbm, xb, sem.at[0])

    lnb = (ln0, ln1, ln2, ln3)
    small = [pltpu.make_async_copy(r, lnb[i], sem.at[1 + i]) for i, r in enumerate((g1, b1, g2, b2))]
    small.append(pltpu.make_async_copy(pos_hbm, posb, sem.at[5]))
    small.append(pltpu.make_async_copy(freq_hbm, freqb, sem.at[6]))

    barrier = pltpu.get_barrier_semaphore()
    greet = [{"tp": partner}]
    for phase in range(2):
        for k in range(1, group_size[phase]):
            greet.append({"dp": peer(phase, k)})
            greet.append({"dp": peer(phase, k), "tp": partner})
    first = [lambda: [copy_x().start()], lambda: [c.start() for c in small],
             lambda: [copy_k().start(priority=1)], lambda: [copy_v().start(priority=1)]]
    first += [lambda c=c: [copy_q(c).start(priority=1)] for c in range(3)]
    first += [lambda c=c: [copy_o(c).start(priority=1)] for c in range(N_O)]
    for i in range(max(len(first), len(greet))):
        if i < len(first):
            first[i]()
        if i < len(greet):
            pl.semaphore_signal(barrier, inc=1, device_id=greet[i], device_id_type=MESH)
    n_peers = len(greet)

    def layer_norm(src, dst, which):
        gain = 1.0 + lnb[2 * which][...].astype(F32).reshape(1, D)
        bias = lnb[2 * which + 1][...].astype(F32).reshape(1, D)
        for i in range(ROWS // 16):
            rows = pl.ds(i * 16, 16)
            v = src[rows, :].astype(F32)
            mean = jnp.mean(v, axis=-1, keepdims=True)
            cen = v - mean
            var = jnp.mean(cen * cen, axis=-1, keepdims=True)
            dst[rows, :] = (cen * lax.rsqrt(var + LN_EPS) * gain + bias).astype(BF16)

    def token_squares(src):
        total = None
        for b in range(ROWS // SEQ):
            acc = None
            for i in range(SEQ // 16):
                hf = src[pl.ds(b * SEQ + i * 16, 16), :].astype(F32)
                part = hf[:8] + hf[8:]
                acc = part if acc is None else acc + part
            mean_tok = jnp.sum(acc, axis=0, keepdims=True) * (1.0 / SEQ)
            sq = mean_tok * mean_tok
            total = sq if total is None else total + sq
        return total

    for c in small:
        c.wait()
    copy_x().wait()
    copy_up(0).start(priority=1)
    copy_up(1).start(priority=1)
    layer_norm(xb, hb, 0)

    diag = (lax.broadcasted_iota(jnp.int32, (SEQ, SEQ), 0)
            == lax.broadcasted_iota(jnp.int32, (SEQ, SEQ), 1))
    pos_row = jnp.broadcast_to(posb[...].astype(F32).reshape(1, SEQ), (SEQ, SEQ))
    pos_col = jnp.sum(jnp.where(diag, pos_row, 0.0), axis=1, keepdims=True)
    angle = pos_col * freqb[...]
    cos, sin = jnp.cos(angle), jnp.sin(angle)
    hl = lax.broadcasted_iota(jnp.int32, (SEQ, HEAD_DIM), 1)
    keep = jnp.where(hl < ROT_DIM, cos, 1.0)
    from_right = jnp.where(hl < ROT_DIM // 2, -sin, 0.0)
    from_left = jnp.where((hl >= ROT_DIM // 2) & (hl < ROT_DIM), sin, 0.0)
    keep = jnp.concatenate([keep, keep], axis=0)
    from_right = jnp.concatenate([from_right, from_right], axis=0)
    from_left = jnp.concatenate([from_left, from_left], axis=0)

    def proj(u):
        return jnp.dot(hb[...], wbuf[pl.ds(u * UNIT, 2 * UNIT), :], preferred_element_type=F32)

    def rope(v):
        u = v.astype(BF16).astype(F32)
        r = pltpu.roll(u, HEAD_DIM - ROT_DIM // 2, 1)
        l = pltpu.roll(u, ROT_DIM // 2, 1)
        return (u * keep + r * from_right + l * from_left).astype(BF16)

    arrive(6, 4, 7)
    copy_up(2).start(priority=1)
    copy_up(3).start(priority=1)
    kk = proj(6)
    vv = proj(8)
    for g in range(4):
        ks[pl.ds(g * ROWS, ROWS), :] = rope(kk[:, g * HEAD_DIM:(g + 1) * HEAD_DIM])
    vs[...] = vv.astype(BF16)
    esc[:, pl.ds(0, D)] = token_squares(hb)

    row = lax.broadcasted_iota(jnp.int32, (3 * ROWS, ROWS), 0) & (ROWS - 1)
    col = lax.broadcasted_iota(jnp.int32, (3 * ROWS, ROWS), 1)
    same = (row >= SEQ) == (col >= SEQ)
    allowed = same & (col <= row)
    blocked = jnp.where(same, F32(-1e30), F32(-jnp.inf))
    lane = lax.broadcasted_iota(jnp.int32, (1, ROWS), 1)

    def attention(g, head_sq):
        q = qs[pl.ds(g * 3 * ROWS, 3 * ROWS), :]
        k = ks[pl.ds(g * ROWS, ROWS), :]
        v = vs[:, g * HEAD_DIM:(g + 1) * HEAD_DIM]
        s = lax.dot_general(q, k, (((1,), (1,)), ((), ())), preferred_element_type=F32) * HEAD_DIM ** -0.5
        s = jnp.where(allowed, s, blocked)
        e = jnp.exp(s - jnp.max(s, axis=-1, keepdims=True))
        p = (e / jnp.sum(e, axis=-1, keepdims=True)).astype(BF16)
        o = jnp.dot(p, v, preferred_element_type=F32).astype(BF16)
        of = o.astype(F32)
        norm = jnp.sqrt(jnp.sum(of * of, axis=-1, keepdims=True))
        for j in range(3):
            i = 3 * g + j
            at[:, i * HEAD_DIM:(i + 1) * HEAD_DIM] = o[j * ROWS:(j + 1) * ROWS, :]
            m0 = jnp.sum(norm[j * ROWS:j * ROWS + SEQ], axis=0, keepdims=True) * (1.0 / SEQ)
            m1 = jnp.sum(norm[j * ROWS + SEQ:(j + 1) * ROWS], axis=0, keepdims=True) * (1.0 / SEQ)
            head_sq = head_sq + jnp.where(lane == i, m0 * m0 + m1 * m1, 0.0)
        return head_sq

    def query(c):
        qq = proj(2 * c)
        for j in range(4):
            qs[pl.ds((4 * c + j) * ROWS, ROWS), :] = rope(qq[:, j * HEAD_DIM:(j + 1) * HEAD_DIM])

    head_sq = jnp.zeros((1, ROWS), F32)
    arrive(0, 4, 8)
    copy_up(4).start(priority=1)
    copy_up(5).start(priority=1)
    query(0)
    query(1)
    head_sq = attention(0, head_sq)
    head_sq = attention(1, head_sq)
    arrive(4, 2, 9)
    copy_up(6).start(priority=1)
    copy_up(7).start(priority=1)
    for r0, n, i in UP_LAST:
        copy_up_last(r0, n, i).start(priority=1)
    query(2)
    head_sq = attention(2, head_sq)
    head_sq = attention(3, head_sq)
    esc[:, pl.ds(D, 128)] = head_sq

    def send(c):
        return pltpu.make_async_remote_copy(
            src_ref=xsend.at[c], dst_ref=xrecv.at[c], send_sem=tp_send, recv_sem=tp_recv.at[TP_SEM[c]],
            device_id={"tp": partner}, device_id_type=MESH)

    def receive(c, n):
        part = pl.ds(c, n)
        pltpu.make_async_remote_copy(
            src_ref=xsend.at[part], dst_ref=xrecv.at[part], send_sem=tp_send, recv_sem=tp_recv.at[TP_SEM[c]],
            device_id={"tp": partner}, device_id_type=MESH).wait_recv()

    pl.semaphore_wait(barrier, n_peers)

    for part in range(2):
        arrive(O_U + 3 * part, 3, 10 + part)
        if part == 0:
            copy_dn(0).start(priority=1)
            copy_dn(1).start(priority=1)
        else:
            copy_dn(2).start(priority=1)
        for c in range(3 * part, 3 * part + 3):
            xsend[c] = jnp.dot(at[...], wbuf[pl.ds((O_U + c) * UNIT, UNIT), :], preferred_element_type=F32)
            send(c).start()
        if part == 1:
            copy_dn(3).start(priority=1)
    for part in range(2):
        receive(3 * part, 3)
        for c in range(3 * part, 3 * part + 3):
            cs = pl.ds(c * CW, CW)
            xm[:, cs] = (xb[:, cs].astype(F32) + (xsend[c] + xrecv[c])).astype(BF16)

    layer_norm(xm, hb, 1)

    def ar_copy(buf, group, phase, src, k):
        return pltpu.make_async_remote_copy(
            src_ref=src, dst_ref=src, send_sem=ar_send.at[group], recv_sem=ar_recv.at[group, phase],
            device_id={"dp": peer(phase, k)}, device_id_type=MESH)

    def ar_start(buf, group, phase, value):
        buf[phase, place[phase]] = value
        for k in range(1, group_size[phase]):
            ar_copy(buf, group, phase, buf.at[phase, place[phase]], k).start()

    def ar_finish(buf, group, phase):
        ar_copy(buf, group, phase, buf.at[phase, pl.ds(0, group_size[phase] - 1)], 1).wait_recv()
        total = buf[phase, 0]
        for j in range(1, group_size[phase]):
            total = total + buf[phase, j]
        return total

    def ar_sent(buf, group):
        ar_copy(buf, group, 0, buf.at[:, pl.ds(0, group_size[0] - 1)], 1).wait_send()

    def e_finish():
        total = jnp.sqrt(ar_finish(are, 0, 1))
        fe_ref[...] = total[:, :D].reshape(D)
        fh_ref[...] = total[:, D:].reshape(128)[:12]

    def na_finish():
        fn_ref[pl.ds(0, NA)] = jnp.sqrt(ar_finish(arn, 1, 1)).reshape(NA)

    NB = FL - NA

    def cross_copy(phase, src, dst, k):
        return pltpu.make_async_remote_copy(
            src_ref=src, dst_ref=dst, send_sem=ar_send.at[3], recv_sem=ar_recv.at[3, phase],
            device_id={"dp": peer(phase, k) if k else dp, "tp": partner}, device_id_type=MESH)

    def cross_start(phase, src):
        for k in range(group_size[phase]):
            cross_copy(phase, src, ars.at[phase, place[phase]], k).start()

    def cross_finish(phase):
        cross_copy(phase, ars.at[phase], ars.at[phase], 0).wait_recv()
        total = ars[phase, 0]
        for j in range(1, group_size[phase]):
            total = total + ars[phase, j]
        return total

    def nb_start():
        @pl.when(tp == 0)
        def _():
            cross_start(0, nsc.at[:, pl.ds(NA, NB)])

        @pl.when(tp == 1)
        def _():
            ar_start(arm, 2, 0, nsc[:, pl.ds(NA, NB)])

    def nb_middle():
        @pl.when(tp == 1)
        def _():
            ar_start(arm, 2, 1, ar_finish(arm, 2, 0))
            stage[...] = cross_finish(0)
            cross_start(1, stage)

    def nb_finish():
        @pl.when(tp == 0)
        def _():
            fn_ref[pl.ds(NA, NB)] = jnp.sqrt(cross_finish(1)).reshape(NB)

        @pl.when(tp == 1)
        def _():
            fn_ref[pl.ds(NA, NB)] = jnp.sqrt(ar_finish(arm, 2, 1)).reshape(NB)
            ar_sent(arm, 2)
        cross_copy(0, ars.at[0], ars.at[0], 0).wait_send()


    def up_score(c, u):
        r = jnp.maximum(u, 0.0)
        a = r * r
        cs = pl.ds(c * CW, CW)
        act[:, cs] = a.astype(BF16)
        m0 = jnp.sum(a[:SEQ], axis=0, keepdims=True) * (1.0 / SEQ)
        m1 = jnp.sum(a[SEQ:], axis=0, keepdims=True) * (1.0 / SEQ)
        nsc[:, cs] = m0 * m0 + m1 * m1

    def up_dot(c):
        return jnp.dot(hb[...], wbuf[pl.ds((UP_U + 2 * c) * UNIT, 2 * UNIT), :], preferred_element_type=F32)

    for i, chunks in enumerate(((0, 1, 2), (3, 4), (5, 6), (7,))):
        arrive(UP_U + 2 * chunks[0], 2 * len(chunks), UP_SEM[chunks[0]])
        if i == 1:
            copy_dn(4).start(priority=1)
            copy_dn(5, 0, 1).start(priority=1)
        elif i == 3:
            copy_dn(5, 1, 1).start(priority=1)
            copy_dn(5, 2, 1).start(priority=1)
        for c in chunks:
            ub[c % 2] = up_dot(c)
            if c not in (0, 5):
                up_score(c - 1, ub[(c - 1) % 2])
        if i == 0:
            esc[:, pl.ds(0, D)] = esc[:, pl.ds(0, D)] + token_squares(hb)
            ar_start(are, 0, 0, esc[...])
        if i == 1:
            up_score(4, ub[0])
            ar_start(arn, 1, 0, nsc[:, pl.ds(0, NA)])
    for r0, n, i in UP_LAST:
        copy_up_last(r0, n, i).wait()
        part = jnp.dot(hb[:, pl.ds(r0, n)], wbuf[pl.ds(r0, n), :], preferred_element_type=F32)
        if r0 == 0:
            ub[(N_UP - 1) % 2] = part
            up_score(N_UP - 2, ub[(N_UP - 2) % 2])
        else:
            up_score(N_UP - 1, ub[(N_UP - 1) % 2] + part)
    nb_start()

    def finish_d(first, n):
        receive(N_O + first, n)
        for c in range(first, first + n):
            cs = pl.ds(c * CW, CW)
            y_ref[:, cs] = (xm[:, cs].astype(F32) + (xsend[N_O + c] + xrecv[N_O + c])).astype(BF16)

    hooks = {
        0: lambda: (ar_start(are, 0, 1, ar_finish(are, 0, 0)), ar_start(arn, 1, 1, ar_finish(arn, 1, 0))),
        2: nb_middle,
        5: lambda: (e_finish(), na_finish()),
    }

    for c in range(N_DN):
        acc = None
        n = DN_U if c < N_DN - 1 else 1
        for u in range(0, DN_U, n):
            copy_dn(c, u, n).wait()
            part = jnp.dot(act[:, pl.ds(u * UNIT, n * UNIT)],
                           wbuf[pl.ds((DN_B + DN_U * c + u) * UNIT, n * UNIT), :],
                           preferred_element_type=F32)
            acc = part if acc is None else acc + part
        xsend[N_O + c] = acc
        send(N_O + c).start()
        if c in (3, 5):
            finish_d(c - 3, 2)
        if c in hooks:
            hooks[c]()
    finish_d(N_DN - 2, 1)
    finish_d(N_DN - 1, 1)
    nb_finish()

    pltpu.make_async_remote_copy(
        src_ref=xsend, dst_ref=xrecv, send_sem=tp_send, recv_sem=tp_recv.at[0],
        device_id={"tp": partner}, device_id_type=MESH).wait_send()
    ar_sent(are, 0)
    ar_sent(arn, 1)


def writer(y, fn, fh, fe, y_out, fn_out, fh_out, fe_out, sem):
    copies = [pltpu.make_async_copy(a, b, sem.at[i])
              for i, (a, b) in enumerate(((y, y_out), (fn, fn_out), (fh, fh_out), (fe, fe_out)))]
    for c in copies:
        c.start()
    for c in copies:
        c.wait()


def solution(mesh):
    dims = (4, 4, 4)

    def local_layer(hidden, positions, ln1_gain, ln1_bias, w_q, w_k, w_v, w_o, ln2_gain, ln2_bias, w_up, w_down):
        hbm = pl.BlockSpec(memory_space=pltpu.HBM)
        vmem = pl.BlockSpec(memory_space=pltpu.VMEM)
        y, fn, fh, fe = pl.pallas_call(
            functools.partial(body, dims),
            out_shape=(
                pltpu.VMEM((ROWS, D), BF16),
                pltpu.VMEM((FL,), F32),
                pltpu.VMEM((12,), F32),
                pltpu.VMEM((D,), F32),
            ),
            in_specs=[hbm] * 13,
            out_specs=(vmem, vmem, vmem, vmem),
            scratch_shapes=[
                pltpu.VMEM((NU * UNIT, CW), BF16),
                pltpu.VMEM((D,), BF16),
                pltpu.VMEM((D,), BF16),
                pltpu.VMEM((D,), BF16),
                pltpu.VMEM((D,), BF16),
                pltpu.VMEM((SEQ,), jnp.int32),
                pltpu.VMEM((1, HEAD_DIM), F32),
                pltpu.VMEM((ROWS, D), BF16),
                pltpu.VMEM((ROWS, D), BF16),
                pltpu.VMEM((ROWS, D), BF16),
                pltpu.VMEM((12 * ROWS, HEAD_DIM), BF16),
                pltpu.VMEM((4 * ROWS, HEAD_DIM), BF16),
                pltpu.VMEM((ROWS, KL), BF16),
                pltpu.VMEM((ROWS, QL), BF16),
                pltpu.VMEM((ROWS, FL), BF16),
                pltpu.VMEM((2, ROWS, CW), F32),
                pltpu.VMEM((N_O + N_DN, ROWS, CW), F32),
                pltpu.VMEM((N_O + N_DN, ROWS, CW), F32),
                pltpu.VMEM((1, FL), F32),
                pltpu.VMEM((1, EH), F32),
                pltpu.VMEM((2, 8, 1, EH), F32),
                pltpu.VMEM((2, 8, 1, NA), F32),
                pltpu.VMEM((2, 8, 1, FL - NA), F32),
                pltpu.VMEM((2, 8, 1, FL - NA), F32),
                pltpu.VMEM((1, FL - NA), F32),
                pltpu.SemaphoreType.DMA((12,)),
                pltpu.SemaphoreType.DMA,
                pltpu.SemaphoreType.DMA((6,)),
                pltpu.SemaphoreType.DMA((4,)),
                pltpu.SemaphoreType.DMA((4, 2)),
            ],
            compiler_params=pltpu.CompilerParams(
                collective_id=0, has_side_effects=True, vmem_limit_bytes=62 * 2**20),
            name="layer",
        )(hidden.reshape(ROWS, D), positions, jnp.asarray(inv_freq_row()), ln1_gain, ln1_bias, ln2_gain, ln2_bias,
          w_q, w_k, w_v, w_o, w_up, w_down)
        held = [pltpu.with_memory_space_constraint(v, pltpu.VMEM) for v in (y, fn, fh, fe)]
        y, fn, fh, fe = pl.pallas_call(
            writer,
            out_shape=tuple(jax.ShapeDtypeStruct(v.shape, v.dtype) for v in held),
            in_specs=[vmem] * 4,
            out_specs=(hbm,) * 4,
            scratch_shapes=[pltpu.SemaphoreType.DMA((4,))],
            name="writer",
        )(*held)
        return y.reshape(hidden.shape), fn, fh, fe

    weight_col = P(None, "tp")
    weight_row = P("tp", None)
    return jax.shard_map(
        local_layer,
        mesh=mesh,
        in_specs=(P("dp"), P(), P(), P(), weight_col, weight_col, weight_col, weight_row, P(), P(), weight_col, weight_row),
        out_specs=(P("dp"), P("tp"), P("tp"), P()),
        check_vma=False,
    )
```
